128 devices in a mesh: member: 32 (over x, y, core), lat: 4 (over z).
Axes of the slice: x: 4, y: 4, z: 4, core: 2. Of those that a mesh axis runs over, the one named last changes fastest.
Arguments:
- ensemble: float32 [64, 3, 1, 128, 1440], P('member', None, None, 'lat'), may hold values from -6 to 6
- observation: float32 [3, 1, 128, 1440], P(None, None, 'lat'), may hold values from -6 to 6
- valid_mask: int32 [64], P('member'), may hold values from 0 to 1, as said below
- band_start: int32 [4], P('lat'), may hold values from 0 to 689
Outputs:
- crps_field: float32 [3, 1, 128, 1440], P(None, None, ('lat', 'member'))
- score_table: float32 [3, 1], replicated
The draws below stay inside these ranges and needn't reach their ends.
Inputs may be any that keep to these rules, and one draw needn't show every extreme that they name: `valid_mask`: exactly 50 entries are 1, at positions drawn afresh.
All inputs are finite; a program needn't handle non-finite values.
Results may differ from the reference program's by a relative error of at most 0.0001.
Values sent between devices are 32-bit elements; how exact they have to be, the bound alone decides.
A program may use at most 64 MiB of HBM per device.

```python
import math
import jax
import jax.numpy as jnp
from jax import lax

GRID_LAT = 721
GRID_LON = 1440
VARS = 3
LEADS = 1
LAT_DEV = 32
MEMBERS = 64
VALID = 50
LAT = 128
N_LAT = 4


def draw_valid_mask(key, part):
    shuffled = jax.random.permutation(jax.random.fold_in(key, 17), MEMBERS)
    return (shuffled < VALID).astype(jnp.int32)


def touch_ends(drawn, key, low, top_value):
    dims = drawn.shape
    spot = [jax.random.randint(jax.random.fold_in(key, axis), (), 0, dims[axis]) for axis in range(len(dims))]
    drawn = drawn.at[tuple(spot)].set(low)
    longest = dims.index(max(dims))
    spot[longest] = (spot[longest] + 1) % dims[longest]
    return drawn.at[tuple(spot)].set(top_value)


def steps_of(stream_key, shape, pieces, low, high):
    gain = 1.0
    for dim, shards_of in pieces:
        steps = jax.random.uniform(jax.random.fold_in(jax.random.fold_in(stream_key, 6), dim), (shards_of,), jnp.float32, low / len(pieces), high / len(pieces))
        gain = gain * jnp.repeat(jnp.exp(steps), shape[dim] // shards_of).reshape((-1,) + (1,) * (len(shape) - 1 - dim))
    return gain


def scatter_about(own_key, extent, scale, bound, split=(), kind=jnp.bfloat16):
    values = scale * jax.random.normal(own_key, extent, jnp.float32)
    if split:
        values = values * steps_of(own_key, extent, split, -0.22, 0.18)
    return jnp.clip(values, -bound, bound).astype(kind)


def setup_inputs(seed: int = 0) -> dict:
    arg_keys = jax.random.split(jax.random.key(seed), 5)
    return {
        "ensemble": scatter_about(arg_keys[0], (MEMBERS, VARS, LEADS, LAT, GRID_LON), 1.0, 6.0, ((0, 32), (3, 4)), jnp.float32),
        "observation": scatter_about(arg_keys[1], (VARS, LEADS, LAT, GRID_LON), 1.0, 6.0, ((2, 4),), jnp.float32),
        "valid_mask": draw_valid_mask(jax.random.fold_in(arg_keys[4], 71), 0),
        "band_start": touch_ends(jax.random.randint(arg_keys[3], (N_LAT,), 0, GRID_LAT - LAT_DEV + 1), jax.random.fold_in(arg_keys[3], 1), 0, GRID_LAT - LAT_DEV).astype(jnp.int32),
    }


def reference(ensemble, observation, valid_mask, band_start):
    member_flags = valid_mask.astype(jnp.float32)
    valid_count = jnp.sum(member_flags)
    flag_column = member_flags[:, None, None, None, None]
    skill_term = jnp.sum(flag_column * jnp.abs(ensemble - observation[None]), axis=0)

    def accumulate(running_sum, block_item):
        member_slab, member_flag = block_item
        distance = jnp.sum(flag_column * jnp.abs(member_slab[None] - ensemble), axis=0)
        return running_sum + member_flag * distance, None

    spread, unused = lax.scan(accumulate, jnp.zeros(observation.shape, jnp.float32), (ensemble, member_flags))
    crps_field = skill_term / valid_count - spread / (2.0 * valid_count * (valid_count - 1.0))
    row_index = (band_start[:, None] + jnp.arange(LAT_DEV, dtype=jnp.int32)[None, :]).reshape(-1).astype(jnp.float32)
    weight = jnp.cos((90.0 - row_index * 180.0 / (GRID_LAT - 1)) * math.pi / 180.0)
    score_table = jnp.sum(crps_field * weight[:, None], axis=(2, 3)) / (N_LAT * LAT_DEV * GRID_LON)
    return (crps_field, score_table)
```

```python
import functools
import math

import jax
import jax.numpy as jnp
from jax import lax
from jax.experimental import pallas as pl
from jax.experimental.pallas import tpu as pltpu
from jax.sharding import Mesh
from jax.sharding import PartitionSpec as P

GRID_LAT = 721
GRID_LON = 1440
VALID = 50
BIG = 1.0e30
MEMBER = ("member_0", "member_1", "member_2")
LAT_MEMBER = ("lat", "member_0", "member_1", "member_2")
AXES = ("member_0", "member_1", "member_2", "lat")
SIZES = {"member_0": 4, "member_1": 4, "member_2": 2, "lat": 4}
MESH_ID = pl.DeviceIdType.MESH

LANES = 128
VARS = 3
FULL = GRID_LON // LANES
TAIL = GRID_LON - FULL * LANES
ROWS = VARS * FULL + 1
SENT = 2 * ROWS
S_STRIDE = 72
R_STRIDE = 80
COLS = 5


def offsets(axes):
    found = [{}]
    for axis in axes:
        found = [dict(o, **{axis: k}) for o in found for k in range(SIZES[axis])]
    found = [o for o in found if any(o.values())]

    def hops(o):
        return sum(min(k, SIZES[a] - k) if a != "member_2" else 0.3 * k for a, k in o.items())

    return sorted(found, key=lambda o: -hops(o))


def peer(offset):
    return {a: lax.rem(lax.axis_index(a) + offset.get(a, 0), SIZES[a]) for a in AXES}


def member_of(coords):
    return (coords["member_0"] * 4 + coords["member_1"]) * 2 + coords["member_2"]


def merge_pairs(lo, n, step, out):
    jump = step * 2
    if jump < n:
        merge_pairs(lo, n, jump, out)
        merge_pairs(lo + step, n, jump, out)
        out.extend((i, i + step) for i in range(lo + step, lo + n - step, jump))
    else:
        out.append((lo, lo + step))


def sort_pairs(lo, n, out):
    if n > 2:
        half = n // 2
        sort_pairs(lo, half, out)
        sort_pairs(lo + half, half, out)
        merge_pairs(lo, n, 1, out)


def pruned(pairs, keep):
    needed = set(range(keep))
    kept = []
    for i, j in reversed(pairs):
        if i in needed or j in needed:
            kept.append((i, j, i in needed, j in needed))
            needed |= {i, j}
    return kept[::-1]


def kernel(
    ens, obs, mask, band, crps_out, score_out,
    xv, ov, sbuf, rbuf, obuf, cbuf, asend, abuf,
    load_sem, obs_sem, send_sem, recv_sem, asend_sem, arecv_sem, ready_sem,
):
    plane = offsets(MEMBER)
    line = offsets(("lat",))
    everyone = offsets(AXES)
    here = {a: lax.axis_index(a) for a in AXES}
    me = member_of(here)

    barrier = pltpu.get_barrier_semaphore()
    for off in plane + line:
        pl.semaphore_signal(barrier, inc=1, device_id=peer(off), device_id_type=MESH_ID)

    load = pltpu.make_async_copy(ens.at[:, :, 0], xv, load_sem)
    load.start()
    tile_row = pl.multiple_of((me // 8) * 8, 8)
    obs_load = pltpu.make_async_copy(obs.at[:, 0, pl.ds(tile_row, 8)], ov, obs_sem)
    obs_load.start()

    flags = [mask[m].astype(jnp.float32) for m in range(2)]
    fills = [(1.0 - f) * BIG for f in flags]
    lane = lax.broadcasted_iota(jnp.int32, (8, LANES), 1)
    load.wait()
    for t in range(4):
        rows = pl.ds(8 * t, 8)

        def put(row, low, high):
            start = 8 * t * S_STRIDE + 2 * row
            sbuf[pl.ds(start, 8, stride=S_STRIDE), :] = low
            sbuf[pl.ds(start + 1, 8, stride=S_STRIDE), :] = high

        tails = []
        for v in range(VARS):
            for c in range(FULL + 1):
                width = LANES if c < FULL else TAIL
                pair = [
                    xv[m, v, rows, pl.ds(c * LANES, width)] * flags[m] + fills[m] for m in range(2)
                ]
                low, high = jnp.minimum(*pair), jnp.maximum(*pair)
                if c < FULL:
                    put(v * FULL + c, low, high)
                else:
                    tails.append((low, high))
        rest = jnp.zeros((8, LANES - VARS * TAIL), jnp.float32)
        put(
            VARS * FULL,
            jnp.concatenate([p[0] for p in tails] + [rest], axis=1),
            jnp.concatenate([p[1] for p in tails] + [rest], axis=1),
        )

    pl.semaphore_wait(barrier, len(plane) + len(line))
    for off in line:
        pl.semaphore_signal(ready_sem, inc=1, device_id=peer(off), device_id_type=MESH_ID)

    copies = []
    for i, off in enumerate(plane):
        target = peer(off)
        start = pl.multiple_of(member_of(target) * S_STRIDE, 8)
        copy = pltpu.make_async_remote_copy(
            src_ref=sbuf.at[pl.ds(start, SENT)],
            dst_ref=rbuf.at[pl.ds(i * R_STRIDE, SENT)],
            send_sem=send_sem,
            recv_sem=recv_sem.at[i],
            device_id=target,
            device_id_type=MESH_ID,
        )
        copy.start()
        copies.append(copy)

    own = pl.multiple_of(me * S_STRIDE, 8)
    rbuf[pl.ds(31 * R_STRIDE, S_STRIDE), :] = sbuf[pl.ds(own, S_STRIDE), :]
    obs_load.wait()
    sub = lax.broadcasted_iota(jnp.int32, (8, LANES), 0)
    chosen = sub == lax.rem(me, 8)
    obs_tails = []
    for v in range(VARS):
        for c in range(FULL):
            part = jnp.where(chosen, ov[v, :, pl.ds(c * LANES, LANES)], 0.0)
            obuf[pl.ds(v * FULL + c, 1), :] = jnp.sum(part, axis=0, keepdims=True)
        part = jnp.where(chosen[:, :TAIL], ov[v, :, pl.ds(FULL * LANES, TAIL)], 0.0)
        obs_tails.append(jnp.sum(part, axis=0, keepdims=True))
    rest = jnp.zeros((1, LANES - VARS * TAIL), jnp.float32)
    obuf[pl.ds(VARS * FULL, 1), :] = jnp.concatenate(obs_tails + [rest], axis=1)
    global_row = (band[0] + me).astype(jnp.float32)
    angle = (90.0 - jnp.full((1, LANES), global_row) * 180.0 / (GRID_LAT - 1)) * math.pi / 180.0
    weight = jnp.cos(angle)

    for copy in copies:
        copy.wait_recv()

    pairs = []
    sort_pairs(0, 64, pairs)
    pairs = pruned(pairs, VALID)

    def column(q, sums):
        vals = [
            rbuf[pl.ds((k // 2) * R_STRIDE + 16 * q + k % 2, 8, stride=2), :] for k in range(64)
        ]
        for i, j, want_low, want_high in pairs:
            a, b = vals[i], vals[j]
            vals[i] = jnp.minimum(a, b) if want_low else None
            vals[j] = jnp.maximum(a, b) if want_high else None
        truth = obuf[pl.ds(pl.multiple_of(8 * q, 8), 8), :]
        skill = [jnp.zeros((8, LANES), jnp.float32) for _ in range(2)]
        spread = [jnp.zeros((8, LANES), jnp.float32) for _ in range(2)]
        for k in range(VALID // 2):
            low, high = vals[k], vals[VALID - 1 - k]
            skill[0] = skill[0] + jnp.abs(low - truth)
            skill[1] = skill[1] + jnp.abs(high - truth)
            spread[k % 2] = spread[k % 2] + (high - low) * float(VALID - 1 - 2 * k)
        crps = (skill[0] + skill[1]) * (1.0 / VALID) - (spread[0] + spread[1]) * (
            1.0 / (VALID * (VALID - 1.0))
        )
        cbuf[pl.ds(pl.multiple_of(8 * q, 8), 8), :] = crps
        row = sub + 8 * q
        result = []
        for v in range(VARS):
            inside = (row >= v * FULL) & (row < (v + 1) * FULL)
            in_tail = (row == VARS * FULL) & (lane >= v * TAIL) & (lane < (v + 1) * TAIL)
            result.append(sums[v] + jnp.where(inside | in_tail, crps, 0.0))
        return tuple(result)

    sums = lax.fori_loop(
        0, COLS, column, tuple(jnp.zeros((8, LANES), jnp.float32) for _ in range(VARS))
    )
    totals = [jnp.sum(s, axis=(0, 1), keepdims=True) for s in sums]
    one_lane = lax.broadcasted_iota(jnp.int32, (1, LANES), 1)
    message = jnp.zeros((1, LANES), jnp.float32)
    for v in range(VARS):
        message = jnp.where(one_lane == v, totals[v] * weight, message)
    my_id = here["lat"] * 32 + me
    asend[0] = message
    abuf[my_id] = message

    pl.semaphore_wait(ready_sem, len(line))
    for off in everyone:
        pltpu.make_async_remote_copy(
            src_ref=asend.at[0],
            dst_ref=abuf.at[my_id],
            send_sem=asend_sem,
            recv_sem=arecv_sem,
            device_id=peer(off),
            device_id_type=MESH_ID,
        ).start()

    for v in range(VARS):
        for c in range(FULL):
            crps_out[v, 0, :, pl.ds(c * LANES, LANES)] = cbuf[pl.ds(v * FULL + c, 1), :]
        last = cbuf[pl.ds(VARS * FULL, 1), :]
        crps_out[v, 0, :, pl.ds(FULL * LANES, TAIL)] = last[:, v * TAIL : (v + 1) * TAIL]

    sent = sbuf.at[pl.ds(0, len(plane) * SENT)]
    pltpu.make_async_copy(sent, sent, send_sem).wait()
    arrived = abuf.at[pl.ds(0, len(everyone))]
    pltpu.make_async_copy(arrived, arrived, arecv_sem).wait()
    total = jnp.sum(abuf[:, 0, :], axis=0, keepdims=True) * (1.0 / (4 * 32 * GRID_LON))
    score_out[...] = total
    pltpu.make_async_copy(arrived, arrived, asend_sem).wait()


def on_device(ensemble, observation, valid_mask, band_start):
    vmem = pl.BlockSpec(memory_space=pltpu.VMEM)
    smem = pl.BlockSpec(memory_space=pltpu.SMEM)
    hbm = pl.BlockSpec(memory_space=pl.ANY)
    crps_field, score = pl.pallas_call(
        kernel,
        out_shape=(
            jax.ShapeDtypeStruct((VARS, 1, 1, GRID_LON), jnp.float32),
            jax.ShapeDtypeStruct((1, LANES), jnp.float32),
        ),
        in_specs=[hbm, hbm, smem, smem],
        out_specs=(vmem, vmem),
        scratch_shapes=[
            pltpu.VMEM((2, VARS, 32, GRID_LON), jnp.float32),
            pltpu.VMEM((VARS, 8, GRID_LON), jnp.float32),
            pltpu.VMEM((32 * S_STRIDE, LANES), jnp.float32),
            pltpu.VMEM((32 * R_STRIDE, LANES), jnp.float32),
            pltpu.VMEM((8 * COLS, LANES), jnp.float32),
            pltpu.VMEM((8 * COLS, LANES), jnp.float32),
            pltpu.VMEM((1, 1, LANES), jnp.float32),
            pltpu.VMEM((128, 1, LANES), jnp.float32),
            pltpu.SemaphoreType.DMA,
            pltpu.SemaphoreType.DMA,
            pltpu.SemaphoreType.DMA,
            pltpu.SemaphoreType.DMA((31,)),
            pltpu.SemaphoreType.DMA,
            pltpu.SemaphoreType.DMA,
            pltpu.SemaphoreType.REGULAR,
        ],
        compiler_params=pltpu.CompilerParams(collective_id=0, has_side_effects=True),
        name="crps",
    )(ensemble, observation, valid_mask, band_start)
    return crps_field, score[0, :VARS].reshape(VARS, 1)


def solution(mesh):
    torus = Mesh(
        mesh.devices.reshape(4, 4, 2, mesh.shape["lat"]),
        ("member_0", "member_1", "member_2", "lat"),
    )
    in_specs = (P(MEMBER, None, None, "lat", None), P(None, None, "lat", None), P(MEMBER), P("lat"))
    out_specs = (P(None, None, LAT_MEMBER, None), P())
    return jax.shard_map(
        on_device, mesh=torus, in_specs=in_specs, out_specs=out_specs, check_vma=False
    )
```

```python
import functools
import math

import jax
import jax.numpy as jnp
from jax import lax
from jax.experimental import pallas as pl
from jax.experimental.pallas import tpu as pltpu
from jax.sharding import Mesh
from jax.sharding import PartitionSpec as P

GRID_LAT = 721
GRID_LON = 1440
VALID = 50
BIG = 1.0e30
MEMBER = ("member_0", "member_1", "member_2")
LAT_MEMBER = ("lat", "member_0", "member_1", "member_2")
AXES = ("member_0", "member_1", "member_2", "lat")
SIZES = {"member_0": 4, "member_1": 4, "member_2": 2, "lat": 4}
MESH_ID = pl.DeviceIdType.MESH

LANES = 128
VARS = 3
FULL = GRID_LON // LANES
TAIL = GRID_LON - FULL * LANES
ROWS = VARS * FULL + 1
SENT = 2 * ROWS
S_STRIDE = 72
R_STRIDE = 80
COLS = 5


def offsets(axes):
    found = [{}]
    for axis in axes:
        found = [dict(o, **{axis: k}) for o in found for k in range(SIZES[axis])]
    found = [o for o in found if any(o.values())]

    def hops(o):
        return sum(min(k, SIZES[a] - k) if a != "member_2" else 0.3 * k for a, k in o.items())

    return sorted(found, key=lambda o: -hops(o))


def peer(offset):
    return {a: lax.rem(lax.axis_index(a) + offset.get(a, 0), SIZES[a]) for a in AXES}


def member_of(coords):
    return (coords["member_0"] * 4 + coords["member_1"]) * 2 + coords["member_2"]


def merge_pairs(lo, n, step, out):
    jump = step * 2
    if jump < n:
        merge_pairs(lo, n, jump, out)
        merge_pairs(lo + step, n, jump, out)
        out.extend((i, i + step) for i in range(lo + step, lo + n - step, jump))
    else:
        out.append((lo, lo + step))


def sort_pairs(lo, n, out):
    if n > 2:
        half = n // 2
        sort_pairs(lo, half, out)
        sort_pairs(lo + half, half, out)
        merge_pairs(lo, n, 1, out)


def pruned(pairs, keep):
    needed = set(range(keep))
    kept = []
    for i, j in reversed(pairs):
        if i in needed or j in needed:
            kept.append((i, j, i in needed, j in needed))
            needed |= {i, j}
    return kept[::-1]


BLOCKS = (2, 1, 3, 0)
PLANE = [[o for o in offsets(MEMBER) if o["member_0"] == dx] for dx in BLOCKS]
LINE = offsets(("lat",))
EVERYONE = offsets(AXES)


def sort_into(vals, pairs):
    for i, j, want_low, want_high in pairs:
        a, b = vals[i], vals[j]
        vals[i] = jnp.minimum(a, b) if want_low else None
        vals[j] = jnp.maximum(a, b) if want_high else None


def kernel(
    ens, obs, mask, band, crps_out, score_out,
    xv, ov, sbuf, rbuf, obuf, cbuf, asend, abuf, mask_s,
    load_sem, obs_sem, flag_sem, send_sem, recv_sem, asend_sem, arecv_sem, ready_sem,
):
    here = {a: lax.axis_index(a) for a in AXES}
    me = member_of(here)

    mask_load = pltpu.make_async_copy(mask, mask_s, flag_sem)
    mask_load.start()
    loads = []
    for k, dx in enumerate(BLOCKS):
        first = pl.multiple_of(lax.rem(here["member_0"] + dx, 4) * 8, 8)
        load = pltpu.make_async_copy(ens.at[:, :, 0, pl.ds(first, 8)], xv.at[k], load_sem.at[k])
        load.start()
        loads.append(load)

    barrier = pltpu.get_barrier_semaphore()
    plane = [o for block in PLANE for o in block]
    for off in offsets(MEMBER) + LINE:
        pl.semaphore_signal(barrier, inc=1, device_id=peer(off), device_id_type=MESH_ID)

    tile_row = pl.multiple_of((me // 8) * 8, 8)
    obs_load = pltpu.make_async_copy(obs.at[:, 0, pl.ds(tile_row, 8)], ov, obs_sem)
    obs_load.start()

    mask_load.wait()
    flags = [mask_s[m].astype(jnp.float32) for m in range(2)]
    fills = [(1.0 - f) * BIG for f in flags]
    lane = lax.broadcasted_iota(jnp.int32, (8, LANES), 1)
    copies = []
    for k, dx in enumerate(BLOCKS):
        loads[k].wait()
        base = lax.rem(here["member_0"] + dx, 4) * (8 * S_STRIDE)

        def put(row, low, high):
            start = base + 2 * row
            sbuf[pl.ds(start, 8, stride=S_STRIDE), :] = low
            sbuf[pl.ds(start + 1, 8, stride=S_STRIDE), :] = high

        tails = []
        for v in range(VARS):
            for c in range(FULL + 1):
                width = LANES if c < FULL else TAIL
                pair = [
                    xv[k, m, v, :, pl.ds(c * LANES, width)] * flags[m] + fills[m] for m in range(2)
                ]
                low, high = jnp.minimum(*pair), jnp.maximum(*pair)
                if c < FULL:
                    put(v * FULL + c, low, high)
                else:
                    tails.append((low, high))
        rest = jnp.zeros((8, LANES - VARS * TAIL), jnp.float32)
        put(
            VARS * FULL,
            jnp.concatenate([p[0] for p in tails] + [rest], axis=1),
            jnp.concatenate([p[1] for p in tails] + [rest], axis=1),
        )

        if k == 0:
            pl.semaphore_wait(barrier, len(plane) + len(LINE))
        for off in PLANE[k]:
            target = peer(off)
            start = pl.multiple_of(member_of(target) * S_STRIDE, 8)
            slot = len(copies)
            copy = pltpu.make_async_remote_copy(
                src_ref=sbuf.at[pl.ds(start, SENT)],
                dst_ref=rbuf.at[pl.ds(slot * R_STRIDE, SENT)],
                send_sem=send_sem,
                recv_sem=recv_sem.at[slot],
                device_id=target,
                device_id_type=MESH_ID,
            )
            copy.start()
            copies.append(copy)

    for off in LINE:
        pl.semaphore_signal(ready_sem, inc=1, device_id=peer(off), device_id_type=MESH_ID)

    own = pl.multiple_of(me * S_STRIDE, 8)
    rbuf[pl.ds(31 * R_STRIDE, S_STRIDE), :] = sbuf[pl.ds(own, S_STRIDE), :]
    obs_load.wait()
    sub = lax.broadcasted_iota(jnp.int32, (8, LANES), 0)
    chosen = sub == lax.rem(me, 8)
    obs_tails = []
    for v in range(VARS):
        for c in range(FULL):
            part = jnp.where(chosen, ov[v, :, pl.ds(c * LANES, LANES)], 0.0)
            obuf[pl.ds(v * FULL + c, 1), :] = jnp.sum(part, axis=0, keepdims=True)
        part = jnp.where(chosen[:, :TAIL], ov[v, :, pl.ds(FULL * LANES, TAIL)], 0.0)
        obs_tails.append(jnp.sum(part, axis=0, keepdims=True))
    rest = jnp.zeros((1, LANES - VARS * TAIL), jnp.float32)
    obuf[pl.ds(VARS * FULL, 1), :] = jnp.concatenate(obs_tails + [rest], axis=1)
    global_row = (band[0] + me).astype(jnp.float32)
    angle = (90.0 - jnp.full((1, LANES), global_row) * 180.0 / (GRID_LAT - 1)) * math.pi / 180.0
    weight = jnp.cos(angle)

    def rows_of(q, k):
        return pl.ds((k // 2) * R_STRIDE + 16 * q + k % 2, 8, stride=2)

    def presort(first, count):
        stage = []
        sort_pairs(0, count, stage)
        stage = pruned(stage, count)

        def column(q, carry):
            vals = [rbuf[rows_of(q, first + k), :] for k in range(count)]
            sort_into(vals, stage)
            for k in range(count):
                rbuf[rows_of(q, first + k), :] = vals[k]
            return carry

        lax.fori_loop(0, COLS, column, 0)

    for copy in copies[:16]:
        copy.wait_recv()
    presort(0, 32)
    for copy in copies[16:24]:
        copy.wait_recv()
    presort(32, 16)
    for copy in copies[24:]:
        copy.wait_recv()

    stage = []
    sort_pairs(48, 16, stage)
    merge_pairs(32, 32, 1, stage)
    merge_pairs(0, 64, 1, stage)
    stage = pruned(stage, VALID)

    def column(q, sums):
        vals = [rbuf[rows_of(q, k), :] for k in range(64)]
        sort_into(vals, stage)
        truth = obuf[pl.ds(pl.multiple_of(8 * q, 8), 8), :]
        skill = [jnp.zeros((8, LANES), jnp.float32) for _ in range(2)]
        spread = [jnp.zeros((8, LANES), jnp.float32) for _ in range(2)]
        for k in range(VALID // 2):
            low, high = vals[k], vals[VALID - 1 - k]
            skill[0] = skill[0] + jnp.abs(low - truth)
            skill[1] = skill[1] + jnp.abs(high - truth)
            spread[k % 2] = spread[k % 2] + (high - low) * float(VALID - 1 - 2 * k)
        crps = (skill[0] + skill[1]) * (1.0 / VALID) - (spread[0] + spread[1]) * (
            1.0 / (VALID * (VALID - 1.0))
        )
        cbuf[pl.ds(pl.multiple_of(8 * q, 8), 8), :] = crps
        row = sub + 8 * q
        result = []
        for v in range(VARS):
            inside = (row >= v * FULL) & (row < (v + 1) * FULL)
            in_tail = (row == VARS * FULL) & (lane >= v * TAIL) & (lane < (v + 1) * TAIL)
            result.append(sums[v] + jnp.where(inside | in_tail, crps, 0.0))
        return tuple(result)

    sums = lax.fori_loop(
        0, COLS, column, tuple(jnp.zeros((8, LANES), jnp.float32) for _ in range(VARS))
    )
    totals = [jnp.sum(s, axis=(0, 1), keepdims=True) for s in sums]
    one_lane = lax.broadcasted_iota(jnp.int32, (1, LANES), 1)
    message = jnp.zeros((1, LANES), jnp.float32)
    for v in range(VARS):
        message = jnp.where(one_lane == v, totals[v] * weight, message)
    my_id = here["lat"] * 32 + me
    asend[0] = message
    abuf[my_id] = message

    pl.semaphore_wait(ready_sem, len(LINE))
    for off in EVERYONE:
        pltpu.make_async_remote_copy(
            src_ref=asend.at[0],
            dst_ref=abuf.at[my_id],
            send_sem=asend_sem,
            recv_sem=arecv_sem,
            device_id=peer(off),
            device_id_type=MESH_ID,
        ).start()

    for v in range(VARS):
        for c in range(FULL):
            crps_out[v, 0, :, pl.ds(c * LANES, LANES)] = cbuf[pl.ds(v * FULL + c, 1), :]
        last = cbuf[pl.ds(VARS * FULL, 1), :]
        crps_out[v, 0, :, pl.ds(FULL * LANES, TAIL)] = last[:, v * TAIL : (v + 1) * TAIL]

    sent = sbuf.at[pl.ds(0, len(plane) * SENT)]
    pltpu.make_async_copy(sent, sent, send_sem).wait()
    arrived = abuf.at[pl.ds(0, len(EVERYONE))]
    pltpu.make_async_copy(arrived, arrived, arecv_sem).wait()
    total = jnp.sum(abuf[:, 0, :], axis=0, keepdims=True) * (1.0 / (4 * 32 * GRID_LON))
    score_out[...] = total
    pltpu.make_async_copy(arrived, arrived, asend_sem).wait()


def write_kernel(crps, score, crps_out, score_out):
    crps_out[...] = crps[...]
    score_out[...] = score[:, :VARS]


def on_device(ensemble, observation, valid_mask, band_start):
    vmem = pl.BlockSpec(memory_space=pltpu.VMEM)
    hbm = pl.BlockSpec(memory_space=pltpu.HBM)
    smem = pl.BlockSpec(memory_space=pltpu.SMEM)
    in_hbm = [
        pltpu.with_memory_space_constraint(a, pltpu.HBM)
        for a in (ensemble, observation, valid_mask)
    ]
    field = jax.ShapeDtypeStruct((VARS, 1, 1, GRID_LON), jnp.float32)
    crps_field, score = pl.pallas_call(
        kernel,
        out_shape=(field, jax.ShapeDtypeStruct((1, LANES), jnp.float32)),
        in_specs=[hbm, hbm, hbm, smem],
        out_specs=(vmem, vmem),
        scratch_shapes=[
            pltpu.VMEM((4, 2, VARS, 8, GRID_LON), jnp.float32),
            pltpu.VMEM((VARS, 8, GRID_LON), jnp.float32),
            pltpu.VMEM((32 * S_STRIDE, LANES), jnp.float32),
            pltpu.VMEM((32 * R_STRIDE, LANES), jnp.float32),
            pltpu.VMEM((8 * COLS, LANES), jnp.float32),
            pltpu.VMEM((8 * COLS, LANES), jnp.float32),
            pltpu.VMEM((1, 1, LANES), jnp.float32),
            pltpu.VMEM((128, 1, LANES), jnp.float32),
            pltpu.SMEM((2,), jnp.int32),
            pltpu.SemaphoreType.DMA((4,)),
            pltpu.SemaphoreType.DMA,
            pltpu.SemaphoreType.DMA,
            pltpu.SemaphoreType.DMA,
            pltpu.SemaphoreType.DMA((31,)),
            pltpu.SemaphoreType.DMA,
            pltpu.SemaphoreType.DMA,
            pltpu.SemaphoreType.REGULAR,
        ],
        compiler_params=pltpu.CompilerParams(
            collective_id=0, has_side_effects=True, vmem_limit_bytes=8 * 1024 * 1024
        ),
        name="crps",
    )(*in_hbm, band_start)
    crps_field, score = pl.pallas_call(
        write_kernel,
        out_shape=(field, jax.ShapeDtypeStruct((1, VARS), jnp.float32)),
        in_specs=[vmem, vmem],
        out_specs=(vmem, vmem),
        compiler_params=pltpu.CompilerParams(vmem_limit_bytes=1024 * 1024),
        name="write",
    )(crps_field, score)
    return crps_field, score.reshape(VARS, 1)


def solution(mesh):
    torus = Mesh(
        mesh.devices.reshape(4, 4, 2, mesh.shape["lat"]),
        ("member_0", "member_1", "member_2", "lat"),
    )
    in_specs = (P(MEMBER, None, None, "lat", None), P(None, None, "lat", None), P(MEMBER), P("lat"))
    out_specs = (P(None, None, LAT_MEMBER, None), P())
    return jax.shard_map(
        on_device, mesh=torus, in_specs=in_specs, out_specs=out_specs, check_vma=False
    )
```

```python
import functools
import math

import jax
import jax.numpy as jnp
from jax import lax
from jax.experimental import pallas as pl
from jax.experimental.pallas import tpu as pltpu
from jax.sharding import Mesh
from jax.sharding import PartitionSpec as P

GRID_LAT = 721
GRID_LON = 1440
VALID = 50
BIG = 1.0e30
MEMBER = ("member_0", "member_1", "member_2")
LAT_MEMBER = ("lat", "member_0", "member_1", "member_2")
AXES = ("member_0", "member_1", "member_2", "lat")
SIZES = {"member_0": 4, "member_1": 4, "member_2": 2, "lat": 4}
MESH_ID = pl.DeviceIdType.MESH

LANES = 128
VARS = 3
FULL = GRID_LON // LANES
TAIL = GRID_LON - FULL * LANES
ROWS = VARS * FULL + 1
SENT = 2 * ROWS
S_STRIDE = 72
R_STRIDE = 80
COLS = 5


def offsets(axes):
    found = [{}]
    for axis in axes:
        found = [dict(o, **{axis: k}) for o in found for k in range(SIZES[axis])]
    found = [o for o in found if any(o.values())]

    def hops(o):
        return sum(min(k, SIZES[a] - k) if a != "member_2" else 0.3 * k for a, k in o.items())

    return sorted(found, key=lambda o: -hops(o))


def chip_hops(o):
    return sum(min(o[a], SIZES[a] - o[a]) for a in ("member_0", "member_1"))


def peer(offset):
    return {a: lax.rem(lax.axis_index(a) + offset.get(a, 0), SIZES[a]) for a in AXES}


def member_of(coords):
    return (coords["member_0"] * 4 + coords["member_1"]) * 2 + coords["member_2"]


def merge_pairs(lo, n, step, out):
    jump = step * 2
    if jump < n:
        merge_pairs(lo, n, jump, out)
        merge_pairs(lo + step, n, jump, out)
        out.extend((i, i + step) for i in range(lo + step, lo + n - step, jump))
    else:
        out.append((lo, lo + step))


def sort_pairs(lo, n, out):
    if n > 2:
        half = n // 2
        sort_pairs(lo, half, out)
        sort_pairs(lo + half, half, out)
        merge_pairs(lo, n, 1, out)


def pruned(pairs, keep):
    needed = set(range(keep))
    kept = []
    for i, j in reversed(pairs):
        if i in needed or j in needed:
            kept.append((i, j, i in needed, j in needed))
            needed |= {i, j}
    return kept[::-1]


BLOCKS = (1, 3, 0, 2)
LEVELS = 2
PLANE = offsets(MEMBER)
NEAR = [o for o in PLANE if o["member_0"] == 0 or o["member_1"] == 0]
SIDE = [o for o in NEAR if o["member_1"] == 0 and o["member_2"] == 0]
FAR = [o for o in PLANE if o not in NEAR]
ROUNDS = (
    [o for o in NEAR if chip_hops(o) == 1],
    FAR + [o for o in NEAR if chip_hops(o) == 2] + [o for o in NEAR if chip_hops(o) == 0],
)
LINE = offsets(("lat",))
EVERYONE = offsets(AXES)


def sort_into(vals, pairs):
    for i, j, want_low, want_high in pairs:
        a, b = vals[i], vals[j]
        vals[i] = jnp.minimum(a, b) if want_low else None
        vals[j] = jnp.maximum(a, b) if want_high else None


def kernel(
    ens, obs, mask, band, crps_out, score_out,
    xv, ov, sbuf, rbuf, obuf, cbuf, asend, abuf, mask_s,
    load_sem, obs_sem, flag_sem, send_sem, recv_sem, asend_sem, arecv_sem, ready_sem, hop_sem,
):
    here = {a: lax.axis_index(a) for a in AXES}
    me = member_of(here)

    mask_load = pltpu.make_async_copy(mask, mask_s, flag_sem)
    mask_load.start()
    loads = []
    for k, dx in enumerate(BLOCKS):
        first = pl.multiple_of(lax.rem(here["member_0"] + dx, 4) * 8, 8)
        load = pltpu.make_async_copy(ens.at[:, :, 0, pl.ds(first, 8)], xv.at[k], load_sem.at[k])
        load.start()
        loads.append(load)

    barrier = pltpu.get_barrier_semaphore()
    for off in NEAR + LINE:
        pl.semaphore_signal(barrier, inc=1, device_id=peer(off), device_id_type=MESH_ID)

    tile_row = pl.multiple_of((me // 8) * 8, 8)
    obs_load = pltpu.make_async_copy(obs.at[:, 0, pl.ds(tile_row, 8)], ov, obs_sem)
    obs_load.start()

    pl.semaphore_wait(barrier, len(NEAR) + len(LINE))

    def pass_on(level):
        for off in SIDE:
            pl.semaphore_signal(
                hop_sem.at[level], inc=1, device_id=peer(off), device_id_type=MESH_ID
            )

    pass_on(0)
    mask_load.wait()
    flags = [mask_s[m].astype(jnp.float32) for m in range(2)]
    fills = [(1.0 - f) * BIG for f in flags]
    lane = lax.broadcasted_iota(jnp.int32, (8, LANES), 1)
    for k, dx in enumerate(BLOCKS):
        loads[k].wait()
        base = lax.rem(here["member_0"] + dx, 4) * (8 * S_STRIDE)

        def put(row, low, high):
            start = base + 2 * row
            sbuf[pl.ds(start, 8, stride=S_STRIDE), :] = low
            sbuf[pl.ds(start + 1, 8, stride=S_STRIDE), :] = high

        tails = []
        for v in range(VARS):
            for c in range(FULL + 1):
                width = LANES if c < FULL else TAIL
                pair = [
                    xv[k, m, v, :, pl.ds(c * LANES, width)] * flags[m] + fills[m] for m in range(2)
                ]
                low, high = jnp.minimum(*pair), jnp.maximum(*pair)
                if c < FULL:
                    put(v * FULL + c, low, high)
                else:
                    tails.append((low, high))
        rest = jnp.zeros((8, LANES - VARS * TAIL), jnp.float32)
        put(
            VARS * FULL,
            jnp.concatenate([p[0] for p in tails] + [rest], axis=1),
            jnp.concatenate([p[1] for p in tails] + [rest], axis=1),
        )

    own = pl.multiple_of(me * S_STRIDE, 8)
    rbuf[pl.ds(0, S_STRIDE), :] = sbuf[pl.ds(own, S_STRIDE), :]
    copies = []
    for level, group in enumerate(ROUNDS):
        if level > 0:
            pl.semaphore_wait(hop_sem.at[level - 1], len(SIDE))
            if level < LEVELS - 1:
                pass_on(level)
        for off in group:
            target = peer(off)
            start = pl.multiple_of(member_of(target) * S_STRIDE, 8)
            slot = len(copies)
            copy = pltpu.make_async_remote_copy(
                src_ref=sbuf.at[pl.ds(start, SENT)],
                dst_ref=rbuf.at[pl.ds((slot + 1) * R_STRIDE, SENT)],
                send_sem=send_sem,
                recv_sem=recv_sem.at[slot],
                device_id=target,
                device_id_type=MESH_ID,
            )
            copy.start()
            copies.append(copy)

    for off in LINE:
        pl.semaphore_signal(ready_sem, inc=1, device_id=peer(off), device_id_type=MESH_ID)

    obs_load.wait()
    sub = lax.broadcasted_iota(jnp.int32, (8, LANES), 0)
    chosen = sub == lax.rem(me, 8)
    obs_tails = []
    for v in range(VARS):
        for c in range(FULL):
            part = jnp.where(chosen, ov[v, :, pl.ds(c * LANES, LANES)], 0.0)
            obuf[pl.ds(v * FULL + c, 1), :] = jnp.sum(part, axis=0, keepdims=True)
        part = jnp.where(chosen[:, :TAIL], ov[v, :, pl.ds(FULL * LANES, TAIL)], 0.0)
        obs_tails.append(jnp.sum(part, axis=0, keepdims=True))
    rest = jnp.zeros((1, LANES - VARS * TAIL), jnp.float32)
    obuf[pl.ds(VARS * FULL, 1), :] = jnp.concatenate(obs_tails + [rest], axis=1)
    global_row = (band[0] + me).astype(jnp.float32)
    angle = (90.0 - jnp.full((1, LANES), global_row) * 180.0 / (GRID_LAT - 1)) * math.pi / 180.0
    weight = jnp.cos(angle)

    def rows_of(q, k):
        return pl.ds((k // 2) * R_STRIDE + 16 * q + k % 2, 8, stride=2)

    def presort(first, count):
        stage = []
        sort_pairs(0, count, stage)
        stage = pruned(stage, count)

        def column(q, carry):
            vals = [rbuf[rows_of(q, first + k), :] for k in range(count)]
            sort_into(vals, stage)
            for k in range(count):
                rbuf[rows_of(q, first + k), :] = vals[k]
            return carry

        lax.fori_loop(0, COLS, column, 0)

    for copy in copies[:15]:
        copy.wait_recv()
    presort(0, 32)
    for copy in copies[15:23]:
        copy.wait_recv()
    presort(32, 16)
    for copy in copies[23:]:
        copy.wait_recv()

    stage = []
    sort_pairs(48, 16, stage)
    merge_pairs(32, 32, 1, stage)
    merge_pairs(0, 64, 1, stage)
    stage = pruned(stage, VALID)

    def column(q, sums):
        vals = [rbuf[rows_of(q, k), :] for k in range(64)]
        sort_into(vals, stage)
        truth = obuf[pl.ds(pl.multiple_of(8 * q, 8), 8), :]
        skill = [jnp.zeros((8, LANES), jnp.float32) for _ in range(2)]
        spread = [jnp.zeros((8, LANES), jnp.float32) for _ in range(2)]
        for k in range(VALID // 2):
            low, high = vals[k], vals[VALID - 1 - k]
            skill[0] = skill[0] + jnp.abs(low - truth)
            skill[1] = skill[1] + jnp.abs(high - truth)
            spread[k % 2] = spread[k % 2] + (high - low) * float(VALID - 1 - 2 * k)
        crps = (skill[0] + skill[1]) * (1.0 / VALID) - (spread[0] + spread[1]) * (
            1.0 / (VALID * (VALID - 1.0))
        )
        cbuf[pl.ds(pl.multiple_of(8 * q, 8), 8), :] = crps
        row = sub + 8 * q
        result = []
        for v in range(VARS):
            inside = (row >= v * FULL) & (row < (v + 1) * FULL)
            in_tail = (row == VARS * FULL) & (lane >= v * TAIL) & (lane < (v + 1) * TAIL)
            result.append(sums[v] + jnp.where(inside | in_tail, crps, 0.0))
        return tuple(result)

    sums = lax.fori_loop(
        0, COLS, column, tuple(jnp.zeros((8, LANES), jnp.float32) for _ in range(VARS))
    )
    totals = [jnp.sum(s, axis=(0, 1), keepdims=True) for s in sums]
    one_lane = lax.broadcasted_iota(jnp.int32, (1, LANES), 1)
    message = jnp.zeros((1, LANES), jnp.float32)
    for v in range(VARS):
        message = jnp.where(one_lane == v, totals[v] * weight, message)
    my_id = here["lat"] * 32 + me
    asend[0] = message
    abuf[my_id] = message

    pl.semaphore_wait(ready_sem, len(LINE))
    for off in EVERYONE:
        pltpu.make_async_remote_copy(
            src_ref=asend.at[0],
            dst_ref=abuf.at[my_id],
            send_sem=asend_sem,
            recv_sem=arecv_sem,
            device_id=peer(off),
            device_id_type=MESH_ID,
        ).start()

    for v in range(VARS):
        for c in range(FULL):
            crps_out[v, 0, :, pl.ds(c * LANES, LANES)] = cbuf[pl.ds(v * FULL + c, 1), :]
        last = cbuf[pl.ds(VARS * FULL, 1), :]
        crps_out[v, 0, :, pl.ds(FULL * LANES, TAIL)] = last[:, v * TAIL : (v + 1) * TAIL]

    sent = sbuf.at[pl.ds(0, len(PLANE) * SENT)]
    pltpu.make_async_copy(sent, sent, send_sem).wait()
    arrived = abuf.at[pl.ds(0, len(EVERYONE))]
    pltpu.make_async_copy(arrived, arrived, arecv_sem).wait()
    total = jnp.sum(abuf[:, 0, :], axis=0, keepdims=True) * (1.0 / (4 * 32 * GRID_LON))
    score_out[...] = total
    pltpu.make_async_copy(arrived, arrived, asend_sem).wait()


def write_kernel(crps, score, crps_out, score_out):
    crps_out[...] = crps[...]
    score_out[...] = score[:, :VARS]


def on_device(ensemble, observation, valid_mask, band_start):
    vmem = pl.BlockSpec(memory_space=pltpu.VMEM)
    hbm = pl.BlockSpec(memory_space=pltpu.HBM)
    smem = pl.BlockSpec(memory_space=pltpu.SMEM)
    in_hbm = [
        pltpu.with_memory_space_constraint(a, pltpu.HBM)
        for a in (ensemble, observation, valid_mask)
    ]
    field = jax.ShapeDtypeStruct((VARS, 1, 1, GRID_LON), jnp.float32)
    crps_field, score = pl.pallas_call(
        kernel,
        out_shape=(field, jax.ShapeDtypeStruct((1, LANES), jnp.float32)),
        in_specs=[hbm, hbm, hbm, smem],
        out_specs=(vmem, vmem),
        scratch_shapes=[
            pltpu.VMEM((4, 2, VARS, 8, GRID_LON), jnp.float32),
            pltpu.VMEM((VARS, 8, GRID_LON), jnp.float32),
            pltpu.VMEM((32 * S_STRIDE, LANES), jnp.float32),
            pltpu.VMEM((32 * R_STRIDE, LANES), jnp.float32),
            pltpu.VMEM((8 * COLS, LANES), jnp.float32),
            pltpu.VMEM((8 * COLS, LANES), jnp.float32),
            pltpu.VMEM((1, 1, LANES), jnp.float32),
            pltpu.VMEM((128, 1, LANES), jnp.float32),
            pltpu.SMEM((2,), jnp.int32),
            pltpu.SemaphoreType.DMA((4,)),
            pltpu.SemaphoreType.DMA,
            pltpu.SemaphoreType.DMA,
            pltpu.SemaphoreType.DMA,
            pltpu.SemaphoreType.DMA((31,)),
            pltpu.SemaphoreType.DMA,
            pltpu.SemaphoreType.DMA,
            pltpu.SemaphoreType.REGULAR,
            pltpu.SemaphoreType.REGULAR((LEVELS - 1,)),
        ],
        compiler_params=pltpu.CompilerParams(
            collective_id=0, has_side_effects=True, vmem_limit_bytes=8 * 1024 * 1024
        ),
        name="crps",
    )(*in_hbm, band_start)
    crps_field, score = pl.pallas_call(
        write_kernel,
        out_shape=(field, jax.ShapeDtypeStruct((1, VARS), jnp.float32)),
        in_specs=[vmem, vmem],
        out_specs=(vmem, vmem),
        compiler_params=pltpu.CompilerParams(vmem_limit_bytes=1024 * 1024),
        name="write",
    )(crps_field, score)
    return crps_field, score.reshape(VARS, 1)


def solution(mesh):
    torus = Mesh(
        mesh.devices.reshape(4, 4, 2, mesh.shape["lat"]),
        ("member_0", "member_1", "member_2", "lat"),
    )
    in_specs = (P(MEMBER, None, None, "lat", None), P(None, None, "lat", None), P(MEMBER), P("lat"))
    out_specs = (P(None, None, LAT_MEMBER, None), P())
    return jax.shard_map(
        on_device, mesh=torus, in_specs=in_specs, out_specs=out_specs, check_vma=False
    )
```

```python
import functools
import math

import jax
import jax.numpy as jnp
from jax import lax
from jax.experimental import pallas as pl
from jax.experimental.pallas import tpu as pltpu
from jax.sharding import Mesh
from jax.sharding import PartitionSpec as P

GRID_LAT = 721
GRID_LON = 1440
VALID = 50
BIG = 1.0e30
MEMBER = ("member_0", "member_1", "member_2")
LAT_MEMBER = ("lat", "member_0", "member_1", "member_2")
AXES = ("member_0", "member_1", "member_2", "lat")
SIZES = {"member_0": 4, "member_1": 4, "member_2": 2, "lat": 4}
MESH_ID = pl.DeviceIdType.MESH

LANES = 128
VARS = 3
FULL = GRID_LON // LANES
TAIL = GRID_LON - FULL * LANES
ROWS = VARS * FULL + 1
SENT = 2 * ROWS
S_STRIDE = 72
R_STRIDE = 80
COLS = 5


def offsets(axes):
    found = [{}]
    for axis in axes:
        found = [dict(o, **{axis: k}) for o in found for k in range(SIZES[axis])]
    found = [o for o in found if any(o.values())]

    def hops(o):
        return sum(min(k, SIZES[a] - k) if a != "member_2" else 0.3 * k for a, k in o.items())

    return sorted(found, key=lambda o: -hops(o))


def chip_hops(o):
    return sum(min(o[a], SIZES[a] - o[a]) for a in ("member_0", "member_1"))


def peer(offset):
    return {a: lax.rem(lax.axis_index(a) + offset.get(a, 0), SIZES[a]) for a in AXES}


def member_of(coords):
    return (coords["member_0"] * 4 + coords["member_1"]) * 2 + coords["member_2"]


def merge_pairs(lo, n, step, out):
    jump = step * 2
    if jump < n:
        merge_pairs(lo, n, jump, out)
        merge_pairs(lo + step, n, jump, out)
        out.extend((i, i + step) for i in range(lo + step, lo + n - step, jump))
    else:
        out.append((lo, lo + step))


def sort_pairs(lo, n, out):
    if n > 2:
        half = n // 2
        sort_pairs(lo, half, out)
        sort_pairs(lo + half, half, out)
        merge_pairs(lo, n, 1, out)


def pruned(pairs, keep):
    needed = set(range(keep))
    kept = []
    for i, j in reversed(pairs):
        if i in needed or j in needed:
            kept.append((i, j, i in needed, j in needed))
            needed |= {i, j}
    return kept[::-1]


BLOCKS = (1, 3, 0, 2)
LEVELS = 2
PLANE = offsets(MEMBER)
NEAR = [o for o in PLANE if o["member_0"] == 0 or o["member_1"] == 0]
SIDE = [o for o in NEAR if o["member_1"] == 0 and o["member_2"] == 0]
FAR = [o for o in PLANE if o not in NEAR]
XY2 = [o for o in NEAR if chip_hops(o) == 2]
C1 = [o for o in NEAR if chip_hops(o) == 0]
D11 = [o for o in FAR if chip_hops(o) == 2]
FARX = [o for o in FAR if chip_hops(o) > 2]
ROUNDS = ([o for o in NEAR if chip_hops(o) == 1], FARX, D11 + XY2 + C1)
RELAY = FAR[:2]
SECOND = 1
LINE = offsets(("lat",))
EVERYONE = offsets(AXES)


def sort_into(vals, pairs):
    for i, j, want_low, want_high in pairs:
        a, b = vals[i], vals[j]
        vals[i] = jnp.minimum(a, b) if want_low else None
        vals[j] = jnp.maximum(a, b) if want_high else None


def kernel(
    ens, obs, mask, band, crps_out, score_out,
    xv, ov, sbuf, rbuf, obuf, cbuf, asend, abuf, mask_s,
    load_sem, obs_sem, flag_sem, send_sem, recv_sem, relay_sem, asend_sem, arecv_sem, ready_sem, line_sem, hop_sem,
):
    here = {a: lax.axis_index(a) for a in AXES}
    me = member_of(here)

    mask_load = pltpu.make_async_copy(mask, mask_s, flag_sem)
    mask_load.start()
    loads = []
    for k, dx in enumerate(BLOCKS):
        first = pl.multiple_of(lax.rem(here["member_0"] + dx, 4) * 8, 8)
        load = pltpu.make_async_copy(ens.at[:, :, 0, pl.ds(first, 8)], xv.at[k], load_sem.at[k])
        load.start()
        loads.append(load)

    barrier = pltpu.get_barrier_semaphore()
    for off in NEAR:
        pl.semaphore_signal(barrier, inc=1, device_id=peer(off), device_id_type=MESH_ID)
    last = here["lat"] // (SIZES["lat"] - 1)
    late = here["lat"] // 2
    mirror = SIZES["lat"] - 1 - here["lat"]

    @pl.when(last == 0)
    def _():
        up = dict(here, lat=SIZES["lat"] - 1)
        pl.semaphore_signal(barrier, inc=1, device_id=up, device_id_type=MESH_ID)

    @pl.when(here["lat"] == 1)
    def _():
        up = dict(here, lat=2)
        pl.semaphore_signal(barrier, inc=1, device_id=up, device_id_type=MESH_ID)

    tile_row = pl.multiple_of((me // 8) * 8, 8)
    obs_load = pltpu.make_async_copy(obs.at[:, 0, pl.ds(tile_row, 8)], ov, obs_sem)
    obs_load.start()

    pl.semaphore_wait(barrier, len(NEAR) + len(LINE) * last + (late - last))

    def pass_on(level):
        for off in SIDE:
            pl.semaphore_signal(
                hop_sem.at[level], inc=1, device_id=peer(off), device_id_type=MESH_ID
            )

    pass_on(0)

    @pl.when(last == 1)
    def _():
        for off in LINE:
            pl.semaphore_signal(line_sem, inc=1, device_id=peer(off), device_id_type=MESH_ID)
    mask_load.wait()
    flags = [mask_s[m].astype(jnp.float32) for m in range(2)]
    fills = [(1.0 - f) * BIG for f in flags]
    lane = lax.broadcasted_iota(jnp.int32, (8, LANES), 1)
    for k, dx in enumerate(BLOCKS):
        loads[k].wait()
        base = lax.rem(here["member_0"] + dx, 4) * (8 * S_STRIDE)

        def put(row, low, high):
            start = base + 2 * row
            sbuf[pl.ds(start, 8, stride=S_STRIDE), :] = low
            sbuf[pl.ds(start + 1, 8, stride=S_STRIDE), :] = high

        tails = []
        for v in range(VARS):
            for c in range(FULL + 1):
                width = LANES if c < FULL else TAIL
                pair = [
                    xv[k, m, v, :, pl.ds(c * LANES, width)] * flags[m] + fills[m] for m in range(2)
                ]
                low, high = jnp.minimum(*pair), jnp.maximum(*pair)
                if c < FULL:
                    put(v * FULL + c, low, high)
                else:
                    tails.append((low, high))
        rest = jnp.zeros((8, LANES - VARS * TAIL), jnp.float32)
        put(
            VARS * FULL,
            jnp.concatenate([p[0] for p in tails] + [rest], axis=1),
            jnp.concatenate([p[1] for p in tails] + [rest], axis=1),
        )

    own = pl.multiple_of(me * S_STRIDE, 8)
    rbuf[pl.ds(0, S_STRIDE), :] = sbuf[pl.ds(own, S_STRIDE), :]
    slots = {}

    def block(place):
        return pl.ds(pl.multiple_of(place * R_STRIDE, 8), SENT)

    def arrived_in(slot, place):
        rows = rbuf.at[block(place)]
        return pltpu.make_async_copy(rows, rows, recv_sem.at[slot])

    def send(group):
        for off in group:
            target = peer(off)
            start = pl.multiple_of(member_of(target) * S_STRIDE, 8)
            slot = slots[str(off)]
            place, flag = slot + 1, slot
            if off in RELAY:
                via = RELAY.index(off)
                moved = late if via < SECOND else last
                stop = dict(here, lat=mirror)
                target = {a: target[a] * (1 - moved) + stop[a] * moved for a in AXES}
                place = place * (1 - moved) + (32 + via) * moved
                flag = flag * (1 - moved) + (31 + via) * moved
            pltpu.make_async_remote_copy(
                src_ref=sbuf.at[pl.ds(start, SENT)],
                dst_ref=rbuf.at[block(place)],
                send_sem=send_sem,
                recv_sem=recv_sem.at[flag],
                device_id=target,
                device_id_type=MESH_ID,
            ).start()

    for level, group in enumerate(ROUNDS):
        if level == 1:
            pl.semaphore_wait(hop_sem.at[level - 1], len(SIDE))
            if level < LEVELS - 1:
                pass_on(level)
        for off in group:
            slots[str(off)] = len(slots)
        if level < 2:
            send(group)

    early = 1 - late if SECOND else 1 - (here["lat"] + SIZES["lat"] - 1) // SIZES["lat"]

    @pl.when(early == 0)
    def _():
        send(ROUNDS[2])

    def forward(via):
        arrived_in(31 + via, 32 + via).wait()
        slot = slots[str(RELAY[via])]
        pltpu.make_async_remote_copy(
            src_ref=rbuf.at[block(32 + via)],
            dst_ref=rbuf.at[block(slot + 1)],
            send_sem=relay_sem.at[via],
            recv_sem=recv_sem.at[slot],
            device_id=dict(peer(RELAY[via]), lat=mirror),
            device_id_type=MESH_ID,
        ).start()

    @pl.when(early == 1)
    def _():
        for via in range(SECOND):
            forward(via)

        @pl.when(here["lat"] == 0)
        def _():
            for via in range(SECOND, len(RELAY)):
                forward(via)

        send(ROUNDS[2])

    @pl.when(last == 0)
    def _():
        pl.semaphore_wait(line_sem, 1)

    for off in LINE:
        pl.semaphore_signal(ready_sem, inc=1, device_id=peer(off), device_id_type=MESH_ID)

    obs_load.wait()
    sub = lax.broadcasted_iota(jnp.int32, (8, LANES), 0)
    chosen = sub == lax.rem(me, 8)
    obs_tails = []
    for v in range(VARS):
        for c in range(FULL):
            part = jnp.where(chosen, ov[v, :, pl.ds(c * LANES, LANES)], 0.0)
            obuf[pl.ds(v * FULL + c, 1), :] = jnp.sum(part, axis=0, keepdims=True)
        part = jnp.where(chosen[:, :TAIL], ov[v, :, pl.ds(FULL * LANES, TAIL)], 0.0)
        obs_tails.append(jnp.sum(part, axis=0, keepdims=True))
    rest = jnp.zeros((1, LANES - VARS * TAIL), jnp.float32)
    obuf[pl.ds(VARS * FULL, 1), :] = jnp.concatenate(obs_tails + [rest], axis=1)
    global_row = (band[0] + me).astype(jnp.float32)
    angle = (90.0 - jnp.full((1, LANES), global_row) * 180.0 / (GRID_LAT - 1)) * math.pi / 180.0
    weight = jnp.cos(angle)

    def rows_of(q, k):
        return pl.ds((k // 2) * R_STRIDE + 16 * q + k % 2, 8, stride=2)

    def presort(first, count):
        stage = []
        sort_pairs(0, count, stage)
        stage = pruned(stage, count)

        def column(q, carry):
            vals = [rbuf[rows_of(q, first + k), :] for k in range(count)]
            sort_into(vals, stage)
            for k in range(count):
                rbuf[rows_of(q, first + k), :] = vals[k]
            return carry

        lax.fori_loop(0, COLS, column, 0)

    for slot in range(15):
        arrived_in(slot, slot + 1).wait()
    presort(0, 32)
    for slot in range(15, 23):
        arrived_in(slot, slot + 1).wait()
    presort(32, 16)
    for slot in range(23, 31):
        arrived_in(slot, slot + 1).wait()

    stage = []
    sort_pairs(48, 16, stage)
    merge_pairs(32, 32, 1, stage)
    merge_pairs(0, 64, 1, stage)
    stage = pruned(stage, VALID)

    def column(q, sums):
        vals = [rbuf[rows_of(q, k), :] for k in range(64)]
        sort_into(vals, stage)
        truth = obuf[pl.ds(pl.multiple_of(8 * q, 8), 8), :]
        skill = [jnp.zeros((8, LANES), jnp.float32) for _ in range(2)]
        spread = [jnp.zeros((8, LANES), jnp.float32) for _ in range(2)]
        for k in range(VALID // 2):
            low, high = vals[k], vals[VALID - 1 - k]
            skill[0] = skill[0] + jnp.abs(low - truth)
            skill[1] = skill[1] + jnp.abs(high - truth)
            spread[k % 2] = spread[k % 2] + (high - low) * float(VALID - 1 - 2 * k)
        crps = (skill[0] + skill[1]) * (1.0 / VALID) - (spread[0] + spread[1]) * (
            1.0 / (VALID * (VALID - 1.0))
        )
        cbuf[pl.ds(pl.multiple_of(8 * q, 8), 8), :] = crps
        row = sub + 8 * q
        result = []
        for v in range(VARS):
            inside = (row >= v * FULL) & (row < (v + 1) * FULL)
            in_tail = (row == VARS * FULL) & (lane >= v * TAIL) & (lane < (v + 1) * TAIL)
            result.append(sums[v] + jnp.where(inside | in_tail, crps, 0.0))
        return tuple(result)

    sums = lax.fori_loop(
        0, COLS, column, tuple(jnp.zeros((8, LANES), jnp.float32) for _ in range(VARS))
    )
    totals = [jnp.sum(s, axis=(0, 1), keepdims=True) for s in sums]
    one_lane = lax.broadcasted_iota(jnp.int32, (1, LANES), 1)
    message = jnp.zeros((1, LANES), jnp.float32)
    for v in range(VARS):
        message = jnp.where(one_lane == v, totals[v] * weight, message)
    my_id = here["lat"] * 32 + me
    asend[0] = message
    abuf[my_id] = message

    pl.semaphore_wait(ready_sem, len(LINE))
    for off in EVERYONE:
        pltpu.make_async_remote_copy(
            src_ref=asend.at[0],
            dst_ref=abuf.at[my_id],
            send_sem=asend_sem,
            recv_sem=arecv_sem,
            device_id=peer(off),
            device_id_type=MESH_ID,
        ).start()

    for v in range(VARS):
        for c in range(FULL):
            crps_out[v, 0, :, pl.ds(c * LANES, LANES)] = cbuf[pl.ds(v * FULL + c, 1), :]
        last = cbuf[pl.ds(VARS * FULL, 1), :]
        crps_out[v, 0, :, pl.ds(FULL * LANES, TAIL)] = last[:, v * TAIL : (v + 1) * TAIL]

    sent = sbuf.at[pl.ds(0, len(PLANE) * SENT)]
    pltpu.make_async_copy(sent, sent, send_sem).wait()
    relayed = rbuf.at[pl.ds(0, SENT)]
    for via in range(len(RELAY)):

        @pl.when(here["lat"] <= (1 if via < SECOND else 0))
        def _():
            pltpu.make_async_copy(relayed, relayed, relay_sem.at[via]).wait()

    arrived = abuf.at[pl.ds(0, len(EVERYONE))]
    pltpu.make_async_copy(arrived, arrived, arecv_sem).wait()
    total = jnp.sum(abuf[:, 0, :], axis=0, keepdims=True) * (1.0 / (4 * 32 * GRID_LON))
    score_out[...] = total
    pltpu.make_async_copy(arrived, arrived, asend_sem).wait()


def write_kernel(crps, score, crps_out, score_out):
    crps_out[...] = crps[...]
    score_out[...] = score[:, :VARS]


def on_device(ensemble, observation, valid_mask, band_start):
    vmem = pl.BlockSpec(memory_space=pltpu.VMEM)
    hbm = pl.BlockSpec(memory_space=pltpu.HBM)
    smem = pl.BlockSpec(memory_space=pltpu.SMEM)
    in_hbm = [
        pltpu.with_memory_space_constraint(a, pltpu.HBM)
        for a in (ensemble, observation, valid_mask)
    ]
    field = jax.ShapeDtypeStruct((VARS, 1, 1, GRID_LON), jnp.float32)
    crps_field, score = pl.pallas_call(
        kernel,
        out_shape=(field, jax.ShapeDtypeStruct((1, LANES), jnp.float32)),
        in_specs=[hbm, hbm, hbm, smem],
        out_specs=(vmem, vmem),
        scratch_shapes=[
            pltpu.VMEM((4, 2, VARS, 8, GRID_LON), jnp.float32),
            pltpu.VMEM((VARS, 8, GRID_LON), jnp.float32),
            pltpu.VMEM((32 * S_STRIDE, LANES), jnp.float32),
            pltpu.VMEM(((32 + len(RELAY)) * R_STRIDE, LANES), jnp.float32),
            pltpu.VMEM((8 * COLS, LANES), jnp.float32),
            pltpu.VMEM((8 * COLS, LANES), jnp.float32),
            pltpu.VMEM((1, 1, LANES), jnp.float32),
            pltpu.VMEM((128, 1, LANES), jnp.float32),
            pltpu.SMEM((2,), jnp.int32),
            pltpu.SemaphoreType.DMA((4,)),
            pltpu.SemaphoreType.DMA,
            pltpu.SemaphoreType.DMA,
            pltpu.SemaphoreType.DMA,
            pltpu.SemaphoreType.DMA((31 + len(RELAY),)),
            pltpu.SemaphoreType.DMA((len(RELAY),)),
            pltpu.SemaphoreType.DMA,
            pltpu.SemaphoreType.DMA,
            pltpu.SemaphoreType.REGULAR,
            pltpu.SemaphoreType.REGULAR,
            pltpu.SemaphoreType.REGULAR((LEVELS - 1,)),
        ],
        compiler_params=pltpu.CompilerParams(
            collective_id=0, has_side_effects=True, vmem_limit_bytes=8 * 1024 * 1024
        ),
        name="crps",
    )(*in_hbm, band_start)
    crps_field, score = pl.pallas_call(
        write_kernel,
        out_shape=(field, jax.ShapeDtypeStruct((1, VARS), jnp.float32)),
        in_specs=[vmem, vmem],
        out_specs=(vmem, vmem),
        compiler_params=pltpu.CompilerParams(vmem_limit_bytes=1024 * 1024),
        name="write",
    )(crps_field, score)
    return crps_field, score.reshape(VARS, 1)


def solution(mesh):
    torus = Mesh(
        mesh.devices.reshape(4, 4, 2, mesh.shape["lat"]),
        ("member_0", "member_1", "member_2", "lat"),
    )
    in_specs = (P(MEMBER, None, None, "lat", None), P(None, None, "lat", None), P(MEMBER), P("lat"))
    out_specs = (P(None, None, LAT_MEMBER, None), P())
    return jax.shard_map(
        on_device, mesh=torus, in_specs=in_specs, out_specs=out_specs, check_vma=False
    )
```

```python
import functools
import math

import jax
import jax.numpy as jnp
from jax import lax
from jax.experimental import pallas as pl
from jax.experimental.pallas import tpu as pltpu
from jax.sharding import Mesh
from jax.sharding import PartitionSpec as P

GRID_LAT = 721
GRID_LON = 1440
VALID = 50
BIG = 1.0e30
MEMBER = ("member_0", "member_1", "member_2")
LAT_MEMBER = ("lat", "member_0", "member_1", "member_2")
AXES = ("member_0", "member_1", "member_2", "lat")
SIZES = {"member_0": 4, "member_1": 4, "member_2": 2, "lat": 4}
MESH_ID = pl.DeviceIdType.MESH

LANES = 128
VARS = 3
FULL = GRID_LON // LANES
TAIL = GRID_LON - FULL * LANES
ROWS = VARS * FULL + 1
SENT = 2 * ROWS
S_STRIDE = 72
R_STRIDE = 80
COLS = 5


def offsets(axes):
    found = [{}]
    for axis in axes:
        found = [dict(o, **{axis: k}) for o in found for k in range(SIZES[axis])]
    found = [o for o in found if any(o.values())]

    def hops(o):
        return sum(min(k, SIZES[a] - k) if a != "member_2" else 0.3 * k for a, k in o.items())

    return sorted(found, key=lambda o: -hops(o))


def chip_hops(o):
    return sum(min(o[a], SIZES[a] - o[a]) for a in ("member_0", "member_1"))


def peer(offset):
    return {a: lax.rem(lax.axis_index(a) + offset.get(a, 0), SIZES[a]) for a in AXES}


def member_of(coords):
    return (coords["member_0"] * 4 + coords["member_1"]) * 2 + coords["member_2"]


def merge_wires(a, b, out):
    if not a or not b:
        return a + b
    if len(a) == 1 and len(b) == 1:
        out.append((a[0], b[0]))
        return [a[0], b[0]]
    even = merge_wires(a[0::2], b[0::2], out)
    odd = merge_wires(a[1::2], b[1::2], out)
    merged = even[:1]
    for i in range(max(len(odd), len(even) - 1)):
        if i < len(odd) and i + 1 < len(even):
            out.append((odd[i], even[i + 1]))
        merged += odd[i : i + 1] + even[i + 1 : i + 2]
    return merged


def sort_wires(wires, out):
    if len(wires) <= 2:
        return wires
    half = (len(wires) + 2) // 4 * 2
    return merge_wires(sort_wires(wires[:half], out), sort_wires(wires[half:], out), out)


def pruned(pairs, keep):
    needed = set(keep)
    kept = []
    for i, j in reversed(pairs):
        if i in needed or j in needed:
            kept.append((i, j, i in needed, j in needed))
            needed |= {i, j}
    return kept[::-1]


BLOCKS = (1, 3, 0, 2)
LEVELS = 2
PLANE = offsets(MEMBER)
NEAR = [o for o in PLANE if o["member_0"] == 0 or o["member_1"] == 0]
SIDE = [o for o in NEAR if o["member_1"] == 0 and o["member_2"] == 0]
FAR = [o for o in PLANE if o not in NEAR]
XY2 = [o for o in NEAR if chip_hops(o) == 2]
C1 = [o for o in NEAR if chip_hops(o) == 0]
D11 = [o for o in FAR if chip_hops(o) == 2]
D3 = [o for o in FAR if chip_hops(o) == 3]
D22 = [o for o in FAR if chip_hops(o) == 4]
N1 = [o for o in NEAR if chip_hops(o) == 1]
ROUNDS = (N1, C1 + D3 + D22, D11 + XY2)
SLOTS = N1 + C1 + D3 + D11 + D22 + XY2
GROUPS = (18, 8, 6)
RELAY = FAR[:2]
SECOND = 1
LINE = offsets(("lat",))
EVERYONE = offsets(AXES)


def sort_into(vals, pairs):
    for i, j, want_low, want_high in pairs:
        a, b = vals[i], vals[j]
        vals[i] = jnp.minimum(a, b) if want_low else None
        vals[j] = jnp.maximum(a, b) if want_high else None


def kernel(
    ens, obs, mask, band, crps_out, score_out,
    xv, ov, sbuf, rbuf, obuf, cbuf, asend, abuf, mask_s,
    load_sem, obs_sem, flag_sem, send_sem, recv_sem, relay_sem, asend_sem, arecv_sem, ready_sem, line_sem, hop_sem,
):
    here = {a: lax.axis_index(a) for a in AXES}
    me = member_of(here)

    mask_load = pltpu.make_async_copy(mask, mask_s, flag_sem)
    mask_load.start()
    loads = []
    for k, dx in enumerate(BLOCKS):
        first = pl.multiple_of(lax.rem(here["member_0"] + dx, 4) * 8, 8)
        load = pltpu.make_async_copy(ens.at[:, :, 0, pl.ds(first, 8)], xv.at[k], load_sem.at[k])
        load.start()
        loads.append(load)

    barrier = pltpu.get_barrier_semaphore()
    for off in NEAR:
        pl.semaphore_signal(barrier, inc=1, device_id=peer(off), device_id_type=MESH_ID)
    last = here["lat"] // (SIZES["lat"] - 1)
    late = here["lat"] // 2
    mirror = SIZES["lat"] - 1 - here["lat"]

    @pl.when(last == 0)
    def _():
        up = dict(here, lat=SIZES["lat"] - 1)
        pl.semaphore_signal(barrier, inc=1, device_id=up, device_id_type=MESH_ID)

    @pl.when(here["lat"] == 1)
    def _():
        up = dict(here, lat=2)
        pl.semaphore_signal(barrier, inc=1, device_id=up, device_id_type=MESH_ID)

    tile_row = pl.multiple_of((me // 8) * 8, 8)
    obs_load = pltpu.make_async_copy(obs.at[:, 0, pl.ds(tile_row, 8)], ov, obs_sem)
    obs_load.start()

    pl.semaphore_wait(barrier, len(NEAR) + len(LINE) * last + (late - last))

    def pass_on(level):
        for off in SIDE:
            pl.semaphore_signal(
                hop_sem.at[level], inc=1, device_id=peer(off), device_id_type=MESH_ID
            )

    pass_on(0)

    @pl.when(last == 1)
    def _():
        for off in LINE:
            pl.semaphore_signal(line_sem, inc=1, device_id=peer(off), device_id_type=MESH_ID)
    mask_load.wait()
    flags = [mask_s[m].astype(jnp.float32) for m in range(2)]
    fills = [(1.0 - f) * BIG for f in flags]
    lane = lax.broadcasted_iota(jnp.int32, (8, LANES), 1)
    for k, dx in enumerate(BLOCKS):
        loads[k].wait()
        base = lax.rem(here["member_0"] + dx, 4) * (8 * S_STRIDE)

        def put(row, low, high):
            start = base + 2 * row
            sbuf[pl.ds(start, 8, stride=S_STRIDE), :] = low
            sbuf[pl.ds(start + 1, 8, stride=S_STRIDE), :] = high

        tails = []
        for v in range(VARS):
            for c in range(FULL + 1):
                width = LANES if c < FULL else TAIL
                pair = [
                    xv[k, m, v, :, pl.ds(c * LANES, width)] * flags[m] + fills[m] for m in range(2)
                ]
                low, high = jnp.minimum(*pair), jnp.maximum(*pair)
                if c < FULL:
                    put(v * FULL + c, low, high)
                else:
                    tails.append((low, high))
        rest = jnp.zeros((8, LANES - VARS * TAIL), jnp.float32)
        put(
            VARS * FULL,
            jnp.concatenate([p[0] for p in tails] + [rest], axis=1),
            jnp.concatenate([p[1] for p in tails] + [rest], axis=1),
        )

    own = pl.multiple_of(me * S_STRIDE, 8)
    rbuf[pl.ds(0, S_STRIDE), :] = sbuf[pl.ds(own, S_STRIDE), :]
    slots = {}

    def block(place):
        return pl.ds(pl.multiple_of(place * R_STRIDE, 8), SENT)

    def arrived_in(slot, place):
        rows = rbuf.at[block(place)]
        return pltpu.make_async_copy(rows, rows, recv_sem.at[slot])

    def send(group):
        for off in group:
            target = peer(off)
            start = pl.multiple_of(member_of(target) * S_STRIDE, 8)
            slot = slots[str(off)]
            place, flag = slot + 1, slot
            if off in RELAY:
                via = RELAY.index(off)
                moved = late if via < SECOND else last
                stop = dict(here, lat=mirror)
                target = {a: target[a] * (1 - moved) + stop[a] * moved for a in AXES}
                place = place * (1 - moved) + (32 + via) * moved
                flag = flag * (1 - moved) + (31 + via) * moved
            pltpu.make_async_remote_copy(
                src_ref=sbuf.at[pl.ds(start, SENT)],
                dst_ref=rbuf.at[block(place)],
                send_sem=send_sem,
                recv_sem=recv_sem.at[flag],
                device_id=target,
                device_id_type=MESH_ID,
            ).start()

    for level, group in enumerate(ROUNDS):
        if level == 1:
            pl.semaphore_wait(hop_sem.at[level - 1], len(SIDE))
            if level < LEVELS - 1:
                pass_on(level)
        for off in group:
            slots[str(off)] = SLOTS.index(off)
        if level < 2:
            send(group)

    early = 1 - late if SECOND else 1 - (here["lat"] + SIZES["lat"] - 1) // SIZES["lat"]

    @pl.when(early == 0)
    def _():
        send(ROUNDS[2])

    def forward(via):
        arrived_in(31 + via, 32 + via).wait()
        slot = slots[str(RELAY[via])]
        pltpu.make_async_remote_copy(
            src_ref=rbuf.at[block(32 + via)],
            dst_ref=rbuf.at[block(slot + 1)],
            send_sem=relay_sem.at[via],
            recv_sem=recv_sem.at[slot],
            device_id=dict(peer(RELAY[via]), lat=mirror),
            device_id_type=MESH_ID,
        ).start()

    @pl.when(early == 1)
    def _():
        for via in range(SECOND):
            forward(via)

        @pl.when(here["lat"] == 0)
        def _():
            for via in range(SECOND, len(RELAY)):
                forward(via)

        send(ROUNDS[2])

    @pl.when(last == 0)
    def _():
        pl.semaphore_wait(line_sem, 1)

    for off in LINE:
        pl.semaphore_signal(ready_sem, inc=1, device_id=peer(off), device_id_type=MESH_ID)

    obs_load.wait()
    sub = lax.broadcasted_iota(jnp.int32, (8, LANES), 0)
    chosen = sub == lax.rem(me, 8)
    obs_tails = []
    for v in range(VARS):
        for c in range(FULL):
            part = jnp.where(chosen, ov[v, :, pl.ds(c * LANES, LANES)], 0.0)
            obuf[pl.ds(v * FULL + c, 1), :] = jnp.sum(part, axis=0, keepdims=True)
        part = jnp.where(chosen[:, :TAIL], ov[v, :, pl.ds(FULL * LANES, TAIL)], 0.0)
        obs_tails.append(jnp.sum(part, axis=0, keepdims=True))
    rest = jnp.zeros((1, LANES - VARS * TAIL), jnp.float32)
    obuf[pl.ds(VARS * FULL, 1), :] = jnp.concatenate(obs_tails + [rest], axis=1)
    global_row = (band[0] + me).astype(jnp.float32)
    angle = (90.0 - jnp.full((1, LANES), global_row) * 180.0 / (GRID_LAT - 1)) * math.pi / 180.0
    weight = jnp.cos(angle)

    def rows_of(q, k):
        return pl.ds((k // 2) * R_STRIDE + 16 * q + k % 2, 8, stride=2)

    order, done = [], 0
    for count in GROUPS:
        for slot in range(max(done, 1), done + count):
            arrived_in(slot - 1, slot).wait()
        stage = []
        fresh = list(range(2 * done, 2 * (done + count)))
        order = merge_wires(order, sort_wires(fresh, stage), stage)
        done += count
        if done == 32:
            break
        stage = pruned(stage, order)

        def presort(q, carry, stage=stage, wires=range(2 * done)):
            vals = [rbuf[rows_of(q, k), :] for k in wires]
            sort_into(vals, stage)
            for k in wires:
                rbuf[rows_of(q, k), :] = vals[k]
            return carry

        lax.fori_loop(0, COLS, presort, 0)

    order = order[:VALID]
    stage = pruned(stage, order)

    def column(q, sums):
        vals = [rbuf[rows_of(q, k), :] for k in range(64)]
        sort_into(vals, stage)
        truth = obuf[pl.ds(pl.multiple_of(8 * q, 8), 8), :]
        skill = [jnp.zeros((8, LANES), jnp.float32) for _ in range(2)]
        spread = [jnp.zeros((8, LANES), jnp.float32) for _ in range(2)]
        for k in range(VALID // 2):
            low, high = vals[order[k]], vals[order[VALID - 1 - k]]
            skill[0] = skill[0] + jnp.abs(low - truth)
            skill[1] = skill[1] + jnp.abs(high - truth)
            spread[k % 2] = spread[k % 2] + (high - low) * float(VALID - 1 - 2 * k)
        crps = (skill[0] + skill[1]) * (1.0 / VALID) - (spread[0] + spread[1]) * (
            1.0 / (VALID * (VALID - 1.0))
        )
        cbuf[pl.ds(pl.multiple_of(8 * q, 8), 8), :] = crps
        row = sub + 8 * q
        result = []
        for v in range(VARS):
            inside = (row >= v * FULL) & (row < (v + 1) * FULL)
            in_tail = (row == VARS * FULL) & (lane >= v * TAIL) & (lane < (v + 1) * TAIL)
            result.append(sums[v] + jnp.where(inside | in_tail, crps, 0.0))
        return tuple(result)

    sums = lax.fori_loop(
        0, COLS, column, tuple(jnp.zeros((8, LANES), jnp.float32) for _ in range(VARS))
    )
    totals = [jnp.sum(s, axis=(0, 1), keepdims=True) for s in sums]
    one_lane = lax.broadcasted_iota(jnp.int32, (1, LANES), 1)
    message = jnp.zeros((1, LANES), jnp.float32)
    for v in range(VARS):
        message = jnp.where(one_lane == v, totals[v] * weight, message)
    my_id = here["lat"] * 32 + me
    asend[0] = message
    abuf[my_id] = message

    pl.semaphore_wait(ready_sem, len(LINE))
    for off in EVERYONE:
        pltpu.make_async_remote_copy(
            src_ref=asend.at[0],
            dst_ref=abuf.at[my_id],
            send_sem=asend_sem,
            recv_sem=arecv_sem,
            device_id=peer(off),
            device_id_type=MESH_ID,
        ).start()

    for v in range(VARS):
        for c in range(FULL):
            crps_out[v, 0, :, pl.ds(c * LANES, LANES)] = cbuf[pl.ds(v * FULL + c, 1), :]
        last = cbuf[pl.ds(VARS * FULL, 1), :]
        crps_out[v, 0, :, pl.ds(FULL * LANES, TAIL)] = last[:, v * TAIL : (v + 1) * TAIL]

    sent = sbuf.at[pl.ds(0, len(PLANE) * SENT)]
    pltpu.make_async_copy(sent, sent, send_sem).wait()
    relayed = rbuf.at[pl.ds(0, SENT)]
    for via in range(len(RELAY)):

        @pl.when(here["lat"] <= (1 if via < SECOND else 0))
        def _():
            pltpu.make_async_copy(relayed, relayed, relay_sem.at[via]).wait()

    arrived = abuf.at[pl.ds(0, len(EVERYONE))]
    pltpu.make_async_copy(arrived, arrived, arecv_sem).wait()
    total = jnp.sum(abuf[:, 0, :], axis=0, keepdims=True) * (1.0 / (4 * 32 * GRID_LON))
    score_out[...] = total
    pltpu.make_async_copy(arrived, arrived, asend_sem).wait()


def write_kernel(crps, score, crps_out, score_out):
    crps_out[...] = crps[...]
    score_out[...] = score[:, :VARS]


def on_device(ensemble, observation, valid_mask, band_start):
    vmem = pl.BlockSpec(memory_space=pltpu.VMEM)
    hbm = pl.BlockSpec(memory_space=pltpu.HBM)
    smem = pl.BlockSpec(memory_space=pltpu.SMEM)
    in_hbm = [
        pltpu.with_memory_space_constraint(a, pltpu.HBM)
        for a in (ensemble, observation, valid_mask)
    ]
    field = jax.ShapeDtypeStruct((VARS, 1, 1, GRID_LON), jnp.float32)
    crps_field, score = pl.pallas_call(
        kernel,
        out_shape=(field, jax.ShapeDtypeStruct((1, LANES), jnp.float32)),
        in_specs=[hbm, hbm, hbm, smem],
        out_specs=(vmem, vmem),
        scratch_shapes=[
            pltpu.VMEM((4, 2, VARS, 8, GRID_LON), jnp.float32),
            pltpu.VMEM((VARS, 8, GRID_LON), jnp.float32),
            pltpu.VMEM((32 * S_STRIDE, LANES), jnp.float32),
            pltpu.VMEM(((32 + len(RELAY)) * R_STRIDE, LANES), jnp.float32),
            pltpu.VMEM((8 * COLS, LANES), jnp.float32),
            pltpu.VMEM((8 * COLS, LANES), jnp.float32),
            pltpu.VMEM((1, 1, LANES), jnp.float32),
            pltpu.VMEM((128, 1, LANES), jnp.float32),
            pltpu.SMEM((2,), jnp.int32),
            pltpu.SemaphoreType.DMA((4,)),
            pltpu.SemaphoreType.DMA,
            pltpu.SemaphoreType.DMA,
            pltpu.SemaphoreType.DMA,
            pltpu.SemaphoreType.DMA((31 + len(RELAY),)),
            pltpu.SemaphoreType.DMA((len(RELAY),)),
            pltpu.SemaphoreType.DMA,
            pltpu.SemaphoreType.DMA,
            pltpu.SemaphoreType.REGULAR,
            pltpu.SemaphoreType.REGULAR,
            pltpu.SemaphoreType.REGULAR((LEVELS - 1,)),
        ],
        compiler_params=pltpu.CompilerParams(
            collective_id=0, has_side_effects=True, vmem_limit_bytes=8 * 1024 * 1024
        ),
        name="crps",
    )(*in_hbm, band_start)
    crps_field, score = pl.pallas_call(
        write_kernel,
        out_shape=(field, jax.ShapeDtypeStruct((1, VARS), jnp.float32)),
        in_specs=[vmem, vmem],
        out_specs=(vmem, vmem),
        compiler_params=pltpu.CompilerParams(vmem_limit_bytes=1024 * 1024),
        name="write",
    )(crps_field, score)
    return crps_field, score.reshape(VARS, 1)


def solution(mesh):
    torus = Mesh(
        mesh.devices.reshape(4, 4, 2, mesh.shape["lat"]),
        ("member_0", "member_1", "member_2", "lat"),
    )
    in_specs = (P(MEMBER, None, None, "lat", None), P(None, None, "lat", None), P(MEMBER), P("lat"))
    out_specs = (P(None, None, LAT_MEMBER, None), P())
    return jax.shard_map(
        on_device, mesh=torus, in_specs=in_specs, out_specs=out_specs, check_vma=False
    )
```

```python
import functools
import math

import jax
import jax.numpy as jnp
from jax import lax
from jax.experimental import pallas as pl
from jax.experimental.pallas import tpu as pltpu
from jax.sharding import Mesh
from jax.sharding import PartitionSpec as P

GRID_LAT = 721
GRID_LON = 1440
VALID = 50
BIG = 1.0e30
MEMBER = ("member_0", "member_1", "member_2")
LAT_MEMBER = ("lat", "member_0", "member_1", "member_2")
AXES = ("member_0", "member_1", "member_2", "lat")
SIZES = {"member_0": 4, "member_1": 4, "member_2": 2, "lat": 4}
MESH_ID = pl.DeviceIdType.MESH

LANES = 128
VARS = 3
FULL = GRID_LON // LANES
TAIL = GRID_LON - FULL * LANES
ROWS = VARS * FULL + 1
SENT = 2 * ROWS
S_STRIDE = 72
R_STRIDE = 80
COLS = 5


def offsets(axes):
    found = [{}]
    for axis in axes:
        found = [dict(o, **{axis: k}) for o in found for k in range(SIZES[axis])]
    found = [o for o in found if any(o.values())]

    def hops(o):
        return sum(min(k, SIZES[a] - k) if a != "member_2" else 0.3 * k for a, k in o.items())

    return sorted(found, key=lambda o: -hops(o))


def chip_hops(o):
    return sum(min(o[a], SIZES[a] - o[a]) for a in ("member_0", "member_1"))


def group_of(place):
    return 0 if place < GROUPS[0] else 1 if place < GROUPS[0] + GROUPS[1] else 2


def peer(offset):
    return {a: lax.rem(lax.axis_index(a) + offset.get(a, 0), SIZES[a]) for a in AXES}


def member_of(coords):
    return (coords["member_0"] * 4 + coords["member_1"]) * 2 + coords["member_2"]


def merge_wires(a, b, out):
    if not a or not b:
        return a + b
    if len(a) == 1 and len(b) == 1:
        out.append((a[0], b[0]))
        return [a[0], b[0]]
    even = merge_wires(a[0::2], b[0::2], out)
    odd = merge_wires(a[1::2], b[1::2], out)
    merged = even[:1]
    for i in range(max(len(odd), len(even) - 1)):
        if i < len(odd) and i + 1 < len(even):
            out.append((odd[i], even[i + 1]))
        merged += odd[i : i + 1] + even[i + 1 : i + 2]
    return merged


def sort_wires(wires, out):
    if len(wires) <= 2:
        return wires
    half = (len(wires) + 2) // 4 * 2
    return merge_wires(sort_wires(wires[:half], out), sort_wires(wires[half:], out), out)


def pruned(pairs, keep):
    needed = set(keep)
    kept = []
    for i, j in reversed(pairs):
        if i in needed or j in needed:
            kept.append((i, j, i in needed, j in needed))
            needed |= {i, j}
    return kept[::-1]


BLOCKS = (1, 3, 0, 2)
LEVELS = 2
PLANE = offsets(MEMBER)
NEAR = [o for o in PLANE if o["member_0"] == 0 or o["member_1"] == 0]
SIDE = [o for o in NEAR if o["member_1"] == 0 and o["member_2"] == 0]
FAR = [o for o in PLANE if o not in NEAR]
XY2 = [o for o in NEAR if chip_hops(o) == 2]
C1 = [o for o in NEAR if chip_hops(o) == 0]
D11 = [o for o in FAR if chip_hops(o) == 2]
D3 = [o for o in FAR if chip_hops(o) == 3]
D22 = [o for o in FAR if chip_hops(o) == 4]
N1 = [o for o in NEAR if chip_hops(o) == 1]
ROUNDS = (N1, C1 + D3 + D22, D11 + XY2)
SLOTS = N1 + C1 + D3 + D11 + D22 + XY2
GROUPS = (18, 8, 6)
RELAY = FAR[:2]
SECOND = 1
LINE = offsets(("lat",))
EVERYONE = offsets(AXES)


def sort_into(vals, pairs):
    for i, j, want_low, want_high in pairs:
        a, b = vals[i], vals[j]
        vals[i] = jnp.minimum(a, b) if want_low else None
        vals[j] = jnp.maximum(a, b) if want_high else None


def kernel(
    ens, obs, mask, band, crps_out, score_out,
    xv, ov, sbuf, rbuf, obuf, cbuf, asend, abuf, mask_s,
    load_sem, obs_sem, flag_sem, send_sem, recv_sem, relay_sem, asend_sem, arecv_sem, ready_sem, line_sem, hop_sem,
):
    here = {a: lax.axis_index(a) for a in AXES}
    me = member_of(here)

    mask_load = pltpu.make_async_copy(mask, mask_s, flag_sem)
    mask_load.start()
    for k, dx in enumerate(BLOCKS):
        first = pl.multiple_of(lax.rem(here["member_0"] + dx, 4) * 8, 8)
        load = pltpu.make_async_copy(ens.at[:, :, 0, pl.ds(first, 8)], xv.at[k], load_sem)
        load.start()

    barrier = pltpu.get_barrier_semaphore()
    for off in NEAR:
        pl.semaphore_signal(barrier, inc=1, device_id=peer(off), device_id_type=MESH_ID)
    last = here["lat"] // (SIZES["lat"] - 1)
    late = here["lat"] // 2
    mirror = SIZES["lat"] - 1 - here["lat"]

    @pl.when(last == 0)
    def _():
        up = dict(here, lat=SIZES["lat"] - 1)
        pl.semaphore_signal(barrier, inc=1, device_id=up, device_id_type=MESH_ID)

    @pl.when(here["lat"] == 1)
    def _():
        up = dict(here, lat=2)
        pl.semaphore_signal(barrier, inc=1, device_id=up, device_id_type=MESH_ID)

    tile_row = pl.multiple_of((me // 8) * 8, 8)
    obs_load = pltpu.make_async_copy(obs.at[:, 0, pl.ds(tile_row, 8)], ov, obs_sem)
    obs_load.start()

    pl.semaphore_wait(barrier, len(NEAR) + len(LINE) * last + (late - last))

    def pass_on(level):
        for off in SIDE:
            pl.semaphore_signal(
                hop_sem.at[level], inc=1, device_id=peer(off), device_id_type=MESH_ID
            )

    pass_on(0)

    @pl.when(last == 1)
    def _():
        for off in LINE:
            pl.semaphore_signal(line_sem, inc=1, device_id=peer(off), device_id_type=MESH_ID)
    mask_load.wait()
    pltpu.make_async_copy(xv, xv, load_sem).wait()
    flags = [mask_s[m].astype(jnp.float32) for m in range(2)]
    fills = [(1.0 - f) * BIG for f in flags]
    lane = lax.broadcasted_iota(jnp.int32, (8, LANES), 1)
    for k, dx in enumerate(BLOCKS):
        base = lax.rem(here["member_0"] + dx, 4) * (8 * S_STRIDE)

        def put(row, low, high):
            start = base + 2 * row
            sbuf[pl.ds(start, 8, stride=S_STRIDE), :] = low
            sbuf[pl.ds(start + 1, 8, stride=S_STRIDE), :] = high

        tails = []
        for v in range(VARS):
            for c in range(FULL + 1):
                width = LANES if c < FULL else TAIL
                pair = [
                    xv[k, m, v, :, pl.ds(c * LANES, width)] * flags[m] + fills[m] for m in range(2)
                ]
                low, high = jnp.minimum(*pair), jnp.maximum(*pair)
                if c < FULL:
                    put(v * FULL + c, low, high)
                else:
                    tails.append((low, high))
        rest = jnp.zeros((8, LANES - VARS * TAIL), jnp.float32)
        put(
            VARS * FULL,
            jnp.concatenate([p[0] for p in tails] + [rest], axis=1),
            jnp.concatenate([p[1] for p in tails] + [rest], axis=1),
        )

    own = pl.multiple_of(me * S_STRIDE, 8)
    rbuf[pl.ds(0, S_STRIDE), :] = sbuf[pl.ds(own, S_STRIDE), :]
    slots = {}

    def block(place):
        return pl.ds(pl.multiple_of(place * R_STRIDE, 8), SENT)

    def await_slots(flag, count):
        rows = rbuf.at[pl.ds(0, count * SENT)]
        pltpu.make_async_copy(rows, rows, recv_sem.at[flag]).wait()

    def send(group):
        for off in group:
            target = peer(off)
            start = pl.multiple_of(member_of(target) * S_STRIDE, 8)
            slot = slots[str(off)]
            place, flag = slot + 1, group_of(slot + 1)
            if off in RELAY:
                via = RELAY.index(off)
                moved = late if via < SECOND else last
                stop = dict(here, lat=mirror)
                target = {a: target[a] * (1 - moved) + stop[a] * moved for a in AXES}
                place = place * (1 - moved) + (32 + via) * moved
                flag = flag * (1 - moved) + (len(GROUPS) + via) * moved
            pltpu.make_async_remote_copy(
                src_ref=sbuf.at[pl.ds(start, SENT)],
                dst_ref=rbuf.at[block(place)],
                send_sem=send_sem,
                recv_sem=recv_sem.at[flag],
                device_id=target,
                device_id_type=MESH_ID,
            ).start()

    for level, group in enumerate(ROUNDS):
        if level == 1:
            pl.semaphore_wait(hop_sem.at[level - 1], len(SIDE))
            if level < LEVELS - 1:
                pass_on(level)
        for off in group:
            slots[str(off)] = SLOTS.index(off)
        if level < 2:
            send(group)

    early = 1 - late if SECOND else 1 - (here["lat"] + SIZES["lat"] - 1) // SIZES["lat"]

    @pl.when(early == 0)
    def _():
        send(ROUNDS[2])

    def forward(via):
        await_slots(len(GROUPS) + via, 1)
        slot = slots[str(RELAY[via])]
        pltpu.make_async_remote_copy(
            src_ref=rbuf.at[block(32 + via)],
            dst_ref=rbuf.at[block(slot + 1)],
            send_sem=relay_sem.at[via],
            recv_sem=recv_sem.at[group_of(slot + 1)],
            device_id=dict(peer(RELAY[via]), lat=mirror),
            device_id_type=MESH_ID,
        ).start()

    @pl.when(early == 1)
    def _():
        for via in range(SECOND):
            forward(via)

        @pl.when(here["lat"] == 0)
        def _():
            for via in range(SECOND, len(RELAY)):
                forward(via)

        send(ROUNDS[2])

    @pl.when(last == 0)
    def _():
        pl.semaphore_wait(line_sem, 1)

    for off in LINE:
        pl.semaphore_signal(ready_sem, inc=1, device_id=peer(off), device_id_type=MESH_ID)

    obs_load.wait()
    sub = lax.broadcasted_iota(jnp.int32, (8, LANES), 0)
    chosen = sub == lax.rem(me, 8)
    obs_tails = []
    for v in range(VARS):
        for c in range(FULL):
            part = jnp.where(chosen, ov[v, :, pl.ds(c * LANES, LANES)], 0.0)
            obuf[pl.ds(v * FULL + c, 1), :] = jnp.sum(part, axis=0, keepdims=True)
        part = jnp.where(chosen[:, :TAIL], ov[v, :, pl.ds(FULL * LANES, TAIL)], 0.0)
        obs_tails.append(jnp.sum(part, axis=0, keepdims=True))
    rest = jnp.zeros((1, LANES - VARS * TAIL), jnp.float32)
    obuf[pl.ds(VARS * FULL, 1), :] = jnp.concatenate(obs_tails + [rest], axis=1)
    global_row = (band[0] + me).astype(jnp.float32)
    angle = (90.0 - jnp.full((1, LANES), global_row) * 180.0 / (GRID_LAT - 1)) * math.pi / 180.0
    weight = jnp.cos(angle)

    def rows_of(q, k):
        return pl.ds((k // 2) * R_STRIDE + 16 * q + k % 2, 8, stride=2)

    order, done = [], 0
    for flag, count in enumerate(GROUPS):
        await_slots(flag, count if done else count - 1)
        stage = []
        fresh = list(range(2 * done, 2 * (done + count)))
        order = merge_wires(order, sort_wires(fresh, stage), stage)
        done += count
        if done == 32:
            break
        stage = pruned(stage, order)

        def presort(q, carry, stage=stage, wires=range(2 * done)):
            vals = [rbuf[rows_of(q, k), :] for k in wires]
            sort_into(vals, stage)
            for k in wires:
                rbuf[rows_of(q, k), :] = vals[k]
            return carry

        lax.fori_loop(0, COLS, presort, 0)

    order = order[:VALID]
    stage = pruned(stage, order)

    def column(q, sums):
        vals = [rbuf[rows_of(q, k), :] for k in range(64)]
        sort_into(vals, stage)
        truth = obuf[pl.ds(pl.multiple_of(8 * q, 8), 8), :]
        skill = [jnp.zeros((8, LANES), jnp.float32) for _ in range(2)]
        spread = [jnp.zeros((8, LANES), jnp.float32) for _ in range(2)]
        for k in range(VALID // 2):
            low, high = vals[order[k]], vals[order[VALID - 1 - k]]
            skill[0] = skill[0] + jnp.abs(low - truth)
            skill[1] = skill[1] + jnp.abs(high - truth)
            spread[k % 2] = spread[k % 2] + (high - low) * float(VALID - 1 - 2 * k)
        crps = (skill[0] + skill[1]) * (1.0 / VALID) - (spread[0] + spread[1]) * (
            1.0 / (VALID * (VALID - 1.0))
        )
        cbuf[pl.ds(pl.multiple_of(8 * q, 8), 8), :] = crps
        row = sub + 8 * q
        result = []
        for v in range(VARS):
            inside = (row >= v * FULL) & (row < (v + 1) * FULL)
            in_tail = (row == VARS * FULL) & (lane >= v * TAIL) & (lane < (v + 1) * TAIL)
            result.append(sums[v] + jnp.where(inside | in_tail, crps, 0.0))
        return tuple(result)

    sums = lax.fori_loop(
        0, COLS, column, tuple(jnp.zeros((8, LANES), jnp.float32) for _ in range(VARS))
    )
    totals = [jnp.sum(s, axis=(0, 1), keepdims=True) for s in sums]
    one_lane = lax.broadcasted_iota(jnp.int32, (1, LANES), 1)
    message = jnp.zeros((1, LANES), jnp.float32)
    for v in range(VARS):
        message = jnp.where(one_lane == v, totals[v] * weight, message)
    my_id = here["lat"] * 32 + me
    asend[0] = message
    abuf[my_id] = message

    pl.semaphore_wait(ready_sem, len(LINE))
    for off in EVERYONE:
        pltpu.make_async_remote_copy(
            src_ref=asend.at[0],
            dst_ref=abuf.at[my_id],
            send_sem=asend_sem,
            recv_sem=arecv_sem,
            device_id=peer(off),
            device_id_type=MESH_ID,
        ).start()

    for v in range(VARS):
        for c in range(FULL):
            crps_out[v, 0, :, pl.ds(c * LANES, LANES)] = cbuf[pl.ds(v * FULL + c, 1), :]
        last = cbuf[pl.ds(VARS * FULL, 1), :]
        crps_out[v, 0, :, pl.ds(FULL * LANES, TAIL)] = last[:, v * TAIL : (v + 1) * TAIL]

    sent = sbuf.at[pl.ds(0, len(PLANE) * SENT)]
    pltpu.make_async_copy(sent, sent, send_sem).wait()
    relayed = rbuf.at[pl.ds(0, SENT)]
    for via in range(len(RELAY)):

        @pl.when(here["lat"] <= (1 if via < SECOND else 0))
        def _():
            pltpu.make_async_copy(relayed, relayed, relay_sem.at[via]).wait()

    arrived = abuf.at[pl.ds(0, len(EVERYONE))]
    pltpu.make_async_copy(arrived, arrived, arecv_sem).wait()
    total = jnp.sum(abuf[:, 0, :], axis=0, keepdims=True) * (1.0 / (4 * 32 * GRID_LON))
    score_out[...] = total
    pltpu.make_async_copy(arrived, arrived, asend_sem).wait()


def write_kernel(crps, score, crps_out, score_out):
    crps_out[...] = crps[...]
    score_out[...] = score[:, :VARS]


def on_device(ensemble, observation, valid_mask, band_start):
    vmem = pl.BlockSpec(memory_space=pltpu.VMEM)
    hbm = pl.BlockSpec(memory_space=pltpu.HBM)
    smem = pl.BlockSpec(memory_space=pltpu.SMEM)
    in_hbm = [
        pltpu.with_memory_space_constraint(a, pltpu.HBM)
        for a in (ensemble, observation, valid_mask)
    ]
    field = jax.ShapeDtypeStruct((VARS, 1, 1, GRID_LON), jnp.float32)
    crps_field, score = pl.pallas_call(
        kernel,
        out_shape=(field, jax.ShapeDtypeStruct((1, LANES), jnp.float32)),
        in_specs=[hbm, hbm, hbm, smem],
        out_specs=(vmem, vmem),
        scratch_shapes=[
            pltpu.VMEM((4, 2, VARS, 8, GRID_LON), jnp.float32),
            pltpu.VMEM((VARS, 8, GRID_LON), jnp.float32),
            pltpu.VMEM((32 * S_STRIDE, LANES), jnp.float32),
            pltpu.VMEM(((32 + len(RELAY)) * R_STRIDE, LANES), jnp.float32),
            pltpu.VMEM((8 * COLS, LANES), jnp.float32),
            pltpu.VMEM((8 * COLS, LANES), jnp.float32),
            pltpu.VMEM((1, 1, LANES), jnp.float32),
            pltpu.VMEM((128, 1, LANES), jnp.float32),
            pltpu.SMEM((2,), jnp.int32),
            pltpu.SemaphoreType.DMA,
            pltpu.SemaphoreType.DMA,
            pltpu.SemaphoreType.DMA,
            pltpu.SemaphoreType.DMA,
            pltpu.SemaphoreType.DMA((len(GROUPS) + len(RELAY),)),
            pltpu.SemaphoreType.DMA((len(RELAY),)),
            pltpu.SemaphoreType.DMA,
            pltpu.SemaphoreType.DMA,
            pltpu.SemaphoreType.REGULAR,
            pltpu.SemaphoreType.REGULAR,
            pltpu.SemaphoreType.REGULAR((LEVELS - 1,)),
        ],
        compiler_params=pltpu.CompilerParams(
            collective_id=0, has_side_effects=True, vmem_limit_bytes=8 * 1024 * 1024
        ),
        name="crps",
    )(*in_hbm, band_start)
    crps_field, score = pl.pallas_call(
        write_kernel,
        out_shape=(field, jax.ShapeDtypeStruct((1, VARS), jnp.float32)),
        in_specs=[vmem, vmem],
        out_specs=(vmem, vmem),
        compiler_params=pltpu.CompilerParams(vmem_limit_bytes=1024 * 1024),
        name="write",
    )(crps_field, score)
    return crps_field, score.reshape(VARS, 1)


def solution(mesh):
    torus = Mesh(
        mesh.devices.reshape(4, 4, 2, mesh.shape["lat"]),
        ("member_0", "member_1", "member_2", "lat"),
    )
    in_specs = (P(MEMBER, None, None, "lat", None), P(None, None, "lat", None), P(MEMBER), P("lat"))
    out_specs = (P(None, None, LAT_MEMBER, None), P())
    return jax.shard_map(
        on_device, mesh=torus, in_specs=in_specs, out_specs=out_specs, check_vma=False
    )
```

```python
import functools
import math

import jax
import jax.numpy as jnp
from jax import lax
from jax.experimental import pallas as pl
from jax.experimental.pallas import tpu as pltpu
from jax.sharding import Mesh
from jax.sharding import PartitionSpec as P

GRID_LAT = 721
GRID_LON = 1440
VALID = 50
BIG = 1.0e30
MEMBER = ("member_0", "member_1", "member_2")
LAT_MEMBER = ("lat", "member_0", "member_1", "member_2")
AXES = ("member_0", "member_1", "member_2", "lat")
SIZES = {"member_0": 4, "member_1": 4, "member_2": 2, "lat": 4}
MESH_ID = pl.DeviceIdType.MESH

LANES = 128
VARS = 3
FULL = GRID_LON // LANES
TAIL = GRID_LON - FULL * LANES
ROWS = VARS * FULL + 1
SENT = 2 * ROWS
S_STRIDE = 72
R_STRIDE = 80
COLS = 5


def offsets(axes):
    found = [{}]
    for axis in axes:
        found = [dict(o, **{axis: k}) for o in found for k in range(SIZES[axis])]
    found = [o for o in found if any(o.values())]

    def hops(o):
        return sum(min(k, SIZES[a] - k) if a != "member_2" else 0.3 * k for a, k in o.items())

    return sorted(found, key=lambda o: -hops(o))


def chip_hops(o):
    return sum(min(o[a], SIZES[a] - o[a]) for a in ("member_0", "member_1"))


def group_of(place):
    return 0 if place < GROUPS[0] else 1 if place < GROUPS[0] + GROUPS[1] else 2


def peer(offset):
    return {a: lax.rem(lax.axis_index(a) + offset.get(a, 0), SIZES[a]) for a in AXES}


def member_of(coords):
    return (coords["member_0"] * 4 + coords["member_1"]) * 2 + coords["member_2"]


def merge_wires(a, b, out):
    if not a or not b:
        return a + b
    if len(a) == 1 and len(b) == 1:
        out.append((a[0], b[0]))
        return [a[0], b[0]]
    even = merge_wires(a[0::2], b[0::2], out)
    odd = merge_wires(a[1::2], b[1::2], out)
    merged = even[:1]
    for i in range(max(len(odd), len(even) - 1)):
        if i < len(odd) and i + 1 < len(even):
            out.append((odd[i], even[i + 1]))
        merged += odd[i : i + 1] + even[i + 1 : i + 2]
    return merged


def sort_wires(wires, out):
    if len(wires) <= 2:
        return wires
    half = (len(wires) + 2) // 4 * 2
    return merge_wires(sort_wires(wires[:half], out), sort_wires(wires[half:], out), out)


def pruned(pairs, keep):
    needed = set(keep)
    kept = []
    for i, j in reversed(pairs):
        if i in needed or j in needed:
            kept.append((i, j, i in needed, j in needed))
            needed |= {i, j}
    return kept[::-1]


BLOCKS = (1, 3, 0, 2)
LEVELS = 2
PLANE = offsets(MEMBER)
NEAR = [o for o in PLANE if o["member_0"] == 0 or o["member_1"] == 0]
SIDE = [o for o in NEAR if o["member_1"] == 0 and o["member_2"] == 0]
FAR = [o for o in PLANE if o not in NEAR]
XY2 = [o for o in NEAR if chip_hops(o) == 2]
C1 = [o for o in NEAR if chip_hops(o) == 0]
D11 = [o for o in FAR if chip_hops(o) == 2]
D3 = [o for o in FAR if chip_hops(o) == 3]
D22 = [o for o in FAR if chip_hops(o) == 4]
N1 = [o for o in NEAR if chip_hops(o) == 1]
ROUNDS = (N1, C1 + D3 + D22, D11 + XY2)
SLOTS = N1 + C1 + D3 + D11 + D22 + XY2
GROUPS = (18, 8, 6)
RELAY = FAR[:2]
SECOND = 1
LINE = offsets(("lat",))
EVERYONE = offsets(AXES)


def sort_into(vals, pairs):
    for i, j, want_low, want_high in pairs:
        a, b = vals[i], vals[j]
        vals[i] = jnp.minimum(a, b) if want_low else None
        vals[j] = jnp.maximum(a, b) if want_high else None


def kernel(
    ens, obs, mask, band, crps_out, score_out,
    xv, ov, sbuf, rbuf, obuf, cbuf, asend, abuf, mask_s,
    load_sem, obs_sem, flag_sem, send_sem, recv_sem, relay_sem, asend_sem, arecv_sem, ready_sem, line_sem, hop_sem,
):
    here = {a: lax.axis_index(a) for a in AXES}
    me = member_of(here)

    mask_load = pltpu.make_async_copy(mask, mask_s, flag_sem)
    mask_load.start()
    for k, dx in enumerate(BLOCKS):
        first = pl.multiple_of(lax.rem(here["member_0"] + dx, 4) * 8, 8)
        load = pltpu.make_async_copy(ens.at[:, :, 0, pl.ds(first, 8)], xv.at[k], load_sem)
        load.start()

    barrier = pltpu.get_barrier_semaphore()
    for off in NEAR:
        pl.semaphore_signal(barrier, inc=1, device_id=peer(off), device_id_type=MESH_ID)
    last = here["lat"] // (SIZES["lat"] - 1)
    late = here["lat"] // 2
    mirror = SIZES["lat"] - 1 - here["lat"]

    @pl.when(last == 0)
    def _():
        up = dict(here, lat=SIZES["lat"] - 1)
        pl.semaphore_signal(barrier, inc=1, device_id=up, device_id_type=MESH_ID)

    @pl.when(here["lat"] == 1)
    def _():
        up = dict(here, lat=2)
        pl.semaphore_signal(barrier, inc=1, device_id=up, device_id_type=MESH_ID)

    tile_row = pl.multiple_of((me // 8) * 8, 8)
    obs_load = pltpu.make_async_copy(obs.at[:, 0, pl.ds(tile_row, 8)], ov, obs_sem)
    obs_load.start()

    pl.semaphore_wait(barrier, len(NEAR) + len(LINE) * last + (late - last))

    def pass_on(level):
        for off in SIDE:
            pl.semaphore_signal(
                hop_sem.at[level], inc=1, device_id=peer(off), device_id_type=MESH_ID
            )

    pass_on(0)

    @pl.when(last == 1)
    def _():
        for off in LINE:
            pl.semaphore_signal(line_sem, inc=1, device_id=peer(off), device_id_type=MESH_ID)
    mask_load.wait()
    pltpu.make_async_copy(xv, xv, load_sem).wait()
    flags = [mask_s[m].astype(jnp.float32) for m in range(2)]
    fills = [(1.0 - f) * BIG for f in flags]
    lane = lax.broadcasted_iota(jnp.int32, (8, LANES), 1)
    for k, dx in enumerate(BLOCKS):
        base = lax.rem(here["member_0"] + dx, 4) * (8 * S_STRIDE)

        def put(row, low, high):
            start = base + 2 * row
            sbuf[pl.ds(start, 8, stride=S_STRIDE), :] = low
            sbuf[pl.ds(start + 1, 8, stride=S_STRIDE), :] = high

        tails = []
        for v in range(VARS):
            for c in range(FULL + 1):
                width = LANES if c < FULL else TAIL
                pair = [
                    xv[k, m, v, :, pl.ds(c * LANES, width)] * flags[m] + fills[m] for m in range(2)
                ]
                low, high = jnp.minimum(*pair), jnp.maximum(*pair)
                if c < FULL:
                    put(v * FULL + c, low, high)
                else:
                    tails.append((low, high))
        rest = jnp.zeros((8, LANES - VARS * TAIL), jnp.float32)
        put(
            VARS * FULL,
            jnp.concatenate([p[0] for p in tails] + [rest], axis=1),
            jnp.concatenate([p[1] for p in tails] + [rest], axis=1),
        )

    own = pl.multiple_of(me * S_STRIDE, 8)
    rbuf[pl.ds(0, S_STRIDE), :] = sbuf[pl.ds(own, S_STRIDE), :]
    slots = {}

    def block(place):
        return pl.ds(pl.multiple_of(place * R_STRIDE, 8), SENT)

    def await_slots(flag, count):
        rows = rbuf.at[pl.ds(0, count * SENT)]
        pltpu.make_async_copy(rows, rows, recv_sem.at[flag]).wait()

    def send(group):
        for off in group:
            target = peer(off)
            start = pl.multiple_of(member_of(target) * S_STRIDE, 8)
            slot = slots[str(off)]
            place, flag = slot + 1, group_of(slot + 1)
            if off in RELAY:
                via = RELAY.index(off)
                moved = late if via < SECOND else last
                stop = dict(here, lat=mirror)
                target = {a: target[a] * (1 - moved) + stop[a] * moved for a in AXES}
                place = place * (1 - moved) + (32 + via) * moved
                flag = flag * (1 - moved) + (len(GROUPS) + via) * moved
            pltpu.make_async_remote_copy(
                src_ref=sbuf.at[pl.ds(start, SENT)],
                dst_ref=rbuf.at[block(place)],
                send_sem=send_sem,
                recv_sem=recv_sem.at[flag],
                device_id=target,
                device_id_type=MESH_ID,
            ).start()

    for level, group in enumerate(ROUNDS):
        if level == 1:
            pl.semaphore_wait(hop_sem.at[level - 1], len(SIDE))
            if level < LEVELS - 1:
                pass_on(level)
        for off in group:
            slots[str(off)] = SLOTS.index(off)
        if level < 2:
            send(group)

    early = 1 - late if SECOND else 1 - (here["lat"] + SIZES["lat"] - 1) // SIZES["lat"]

    @pl.when(early == 0)
    def _():
        send(ROUNDS[2])

    def forward(via):
        await_slots(len(GROUPS) + via, 1)
        slot = slots[str(RELAY[via])]
        pltpu.make_async_remote_copy(
            src_ref=rbuf.at[block(32 + via)],
            dst_ref=rbuf.at[block(slot + 1)],
            send_sem=relay_sem.at[via],
            recv_sem=recv_sem.at[group_of(slot + 1)],
            device_id=dict(peer(RELAY[via]), lat=mirror),
            device_id_type=MESH_ID,
        ).start()

    @pl.when(early == 1)
    def _():
        for via in range(SECOND):
            forward(via)

        @pl.when(here["lat"] == 0)
        def _():
            for via in range(SECOND, len(RELAY)):
                forward(via)

        send(ROUNDS[2])

    @pl.when(last == 0)
    def _():
        pl.semaphore_wait(line_sem, 1)

    for off in LINE:
        pl.semaphore_signal(ready_sem, inc=1, device_id=peer(off), device_id_type=MESH_ID)

    obs_load.wait()
    sub = lax.broadcasted_iota(jnp.int32, (8, LANES), 0)
    chosen = sub == lax.rem(me, 8)
    obs_tails = []
    for v in range(VARS):
        for c in range(FULL):
            part = jnp.where(chosen, ov[v, :, pl.ds(c * LANES, LANES)], 0.0)
            obuf[pl.ds(v * FULL + c, 1), :] = jnp.sum(part, axis=0, keepdims=True)
        part = jnp.where(chosen[:, :TAIL], ov[v, :, pl.ds(FULL * LANES, TAIL)], 0.0)
        obs_tails.append(jnp.sum(part, axis=0, keepdims=True))
    rest = jnp.zeros((1, LANES - VARS * TAIL), jnp.float32)
    obuf[pl.ds(VARS * FULL, 1), :] = jnp.concatenate(obs_tails + [rest], axis=1)
    global_row = (band[0] + me).astype(jnp.float32)
    angle = (90.0 - jnp.full((1, LANES), global_row) * 180.0 / (GRID_LAT - 1)) * math.pi / 180.0
    weight = jnp.cos(angle)

    def rows_of(q, k):
        return pl.ds((k // 2) * R_STRIDE + 16 * q + k % 2, 8, stride=2)

    order, done = [], 0
    for flag, count in enumerate(GROUPS):
        await_slots(flag, count if done else count - 1)
        stage = []
        fresh = list(range(2 * done, 2 * (done + count)))
        order = merge_wires(order, sort_wires(fresh, stage), stage)
        done += count
        if done == 32:
            break
        stage = pruned(stage, order)

        def presort(q, carry, stage=stage, wires=range(2 * done)):
            vals = [rbuf[rows_of(q, k), :] for k in wires]
            sort_into(vals, stage)
            for k in wires:
                rbuf[rows_of(q, k), :] = vals[k]
            return carry

        lax.fori_loop(0, COLS, presort, 0)

    order = order[:VALID]
    stage = pruned(stage, order)

    def column(q, sums):
        vals = [rbuf[rows_of(q, k), :] for k in range(64)]
        sort_into(vals, stage)
        truth = obuf[pl.ds(pl.multiple_of(8 * q, 8), 8), :]
        skill = [jnp.zeros((8, LANES), jnp.float32) for _ in range(2)]
        spread = [jnp.zeros((8, LANES), jnp.float32) for _ in range(2)]
        for k in range(VALID // 2):
            low, high = vals[order[k]], vals[order[VALID - 1 - k]]
            skill[0] = skill[0] + jnp.abs(low - truth)
            skill[1] = skill[1] + jnp.abs(high - truth)
            spread[k % 2] = spread[k % 2] + (high - low) * float(VALID - 1 - 2 * k)
        crps = (skill[0] + skill[1]) * (1.0 / VALID) - (spread[0] + spread[1]) * (
            1.0 / (VALID * (VALID - 1.0))
        )
        cbuf[pl.ds(pl.multiple_of(8 * q, 8), 8), :] = crps
        row = sub + 8 * q
        result = []
        for v in range(VARS):
            inside = (row >= v * FULL) & (row < (v + 1) * FULL)
            in_tail = (row == VARS * FULL) & (lane >= v * TAIL) & (lane < (v + 1) * TAIL)
            result.append(sums[v] + jnp.where(inside | in_tail, crps, 0.0))
        return tuple(result)

    sums = lax.fori_loop(
        0, COLS, column, tuple(jnp.zeros((8, LANES), jnp.float32) for _ in range(VARS))
    )
    totals = [jnp.sum(s, axis=(0, 1), keepdims=True) for s in sums]
    one_lane = lax.broadcasted_iota(jnp.int32, (1, LANES), 1)
    message = jnp.zeros((1, LANES), jnp.float32)
    for v in range(VARS):
        message = jnp.where(one_lane == v, totals[v] * weight, message)
    my_id = here["lat"] * 32 + me
    asend[0] = message
    abuf[my_id] = message

    pl.semaphore_wait(ready_sem, len(LINE))
    targets = [dict(peer(off), lat=z) for z in range(SIZES["lat"]) for off in PLANE]
    for target in targets + [peer(off) for off in LINE]:
        pltpu.make_async_remote_copy(
            src_ref=asend.at[0],
            dst_ref=abuf.at[my_id],
            send_sem=asend_sem,
            recv_sem=arecv_sem,
            device_id=target,
            device_id_type=MESH_ID,
        ).start()

    for v in range(VARS):
        for c in range(FULL):
            crps_out[v, 0, :, pl.ds(c * LANES, LANES)] = cbuf[pl.ds(v * FULL + c, 1), :]
        last = cbuf[pl.ds(VARS * FULL, 1), :]
        crps_out[v, 0, :, pl.ds(FULL * LANES, TAIL)] = last[:, v * TAIL : (v + 1) * TAIL]

    sent = sbuf.at[pl.ds(0, len(PLANE) * SENT)]
    pltpu.make_async_copy(sent, sent, send_sem).wait()
    relayed = rbuf.at[pl.ds(0, SENT)]
    for via in range(len(RELAY)):

        @pl.when(here["lat"] <= (1 if via < SECOND else 0))
        def _():
            pltpu.make_async_copy(relayed, relayed, relay_sem.at[via]).wait()

    arrived = abuf.at[pl.ds(0, len(EVERYONE))]
    pltpu.make_async_copy(arrived, arrived, arecv_sem).wait()
    total = jnp.sum(abuf[:, 0, :], axis=0, keepdims=True) * (1.0 / (4 * 32 * GRID_LON))
    score_out[...] = total
    pltpu.make_async_copy(arrived, arrived, asend_sem).wait()


def write_kernel(crps, score, crps_out, score_out):
    crps_out[...] = crps[...]
    score_out[...] = score[:, :VARS]


def on_device(ensemble, observation, valid_mask, band_start):
    vmem = pl.BlockSpec(memory_space=pltpu.VMEM)
    hbm = pl.BlockSpec(memory_space=pltpu.HBM)
    smem = pl.BlockSpec(memory_space=pltpu.SMEM)
    in_hbm = [
        pltpu.with_memory_space_constraint(a, pltpu.HBM)
        for a in (ensemble, observation, valid_mask)
    ]
    field = jax.ShapeDtypeStruct((VARS, 1, 1, GRID_LON), jnp.float32)
    crps_field, score = pl.pallas_call(
        kernel,
        out_shape=(field, jax.ShapeDtypeStruct((1, LANES), jnp.float32)),
        in_specs=[hbm, hbm, hbm, smem],
        out_specs=(vmem, vmem),
        scratch_shapes=[
            pltpu.VMEM((4, 2, VARS, 8, GRID_LON), jnp.float32),
            pltpu.VMEM((VARS, 8, GRID_LON), jnp.float32),
            pltpu.VMEM((32 * S_STRIDE, LANES), jnp.float32),
            pltpu.VMEM(((32 + len(RELAY)) * R_STRIDE, LANES), jnp.float32),
            pltpu.VMEM((8 * COLS, LANES), jnp.float32),
            pltpu.VMEM((8 * COLS, LANES), jnp.float32),
            pltpu.VMEM((1, 1, LANES), jnp.float32),
            pltpu.VMEM((128, 1, LANES), jnp.float32),
            pltpu.SMEM((2,), jnp.int32),
            pltpu.SemaphoreType.DMA,
            pltpu.SemaphoreType.DMA,
            pltpu.SemaphoreType.DMA,
            pltpu.SemaphoreType.DMA,
            pltpu.SemaphoreType.DMA((len(GROUPS) + len(RELAY),)),
            pltpu.SemaphoreType.DMA((len(RELAY),)),
            pltpu.SemaphoreType.DMA,
            pltpu.SemaphoreType.DMA,
            pltpu.SemaphoreType.REGULAR,
            pltpu.SemaphoreType.REGULAR,
            pltpu.SemaphoreType.REGULAR((LEVELS - 1,)),
        ],
        compiler_params=pltpu.CompilerParams(
            collective_id=0, has_side_effects=True, vmem_limit_bytes=8 * 1024 * 1024
        ),
        name="crps",
    )(*in_hbm, band_start)
    crps_field, score = pl.pallas_call(
        write_kernel,
        out_shape=(field, jax.ShapeDtypeStruct((1, VARS), jnp.float32)),
        in_specs=[vmem, vmem],
        out_specs=(vmem, vmem),
        compiler_params=pltpu.CompilerParams(vmem_limit_bytes=1024 * 1024),
        name="write",
    )(crps_field, score)
    return crps_field, score.reshape(VARS, 1)


def solution(mesh):
    torus = Mesh(
        mesh.devices.reshape(4, 4, 2, mesh.shape["lat"]),
        ("member_0", "member_1", "member_2", "lat"),
    )
    in_specs = (P(MEMBER, None, None, "lat", None), P(None, None, "lat", None), P(MEMBER), P("lat"))
    out_specs = (P(None, None, LAT_MEMBER, None), P())
    return jax.shard_map(
        on_device, mesh=torus, in_specs=in_specs, out_specs=out_specs, check_vma=False
    )
```

```python
import functools
import math

import jax
import jax.numpy as jnp
from jax import lax
from jax.experimental import pallas as pl
from jax.experimental.pallas import tpu as pltpu
from jax.sharding import Mesh
from jax.sharding import PartitionSpec as P

GRID_LAT = 721
GRID_LON = 1440
VALID = 50
BIG = 1.0e30
MEMBER = ("member_0", "member_1", "member_2")
LAT_MEMBER = ("lat", "member_0", "member_1", "member_2")
AXES = ("member_0", "member_1", "member_2", "lat")
SIZES = {"member_0": 4, "member_1": 4, "member_2": 2, "lat": 4}
MESH_ID = pl.DeviceIdType.MESH

LANES = 128
VARS = 3
FULL = GRID_LON // LANES
TAIL = GRID_LON - FULL * LANES
ROWS = VARS * FULL + 1
SENT = 2 * ROWS
S_STRIDE = 72
R_STRIDE = 80
COLS = 5


def offsets(axes):
    found = [{}]
    for axis in axes:
        found = [dict(o, **{axis: k}) for o in found for k in range(SIZES[axis])]
    found = [o for o in found if any(o.values())]

    def hops(o):
        return sum(min(k, SIZES[a] - k) if a != "member_2" else 0.3 * k for a, k in o.items())

    return sorted(found, key=lambda o: -hops(o))


def chip_hops(o):
    return sum(min(o[a], SIZES[a] - o[a]) for a in ("member_0", "member_1"))


def group_of(place):
    return 0 if place < GROUPS[0] else 1 if place < GROUPS[0] + GROUPS[1] else 2


def peer(offset):
    return {a: lax.rem(lax.axis_index(a) + offset.get(a, 0), SIZES[a]) for a in AXES}


def member_of(coords):
    return (coords["member_0"] * 4 + coords["member_1"]) * 2 + coords["member_2"]


def merge_wires(a, b, out):
    if not a or not b:
        return a + b
    if len(a) == 1 and len(b) == 1:
        out.append((a[0], b[0]))
        return [a[0], b[0]]
    even = merge_wires(a[0::2], b[0::2], out)
    odd = merge_wires(a[1::2], b[1::2], out)
    merged = even[:1]
    for i in range(max(len(odd), len(even) - 1)):
        if i < len(odd) and i + 1 < len(even):
            out.append((odd[i], even[i + 1]))
        merged += odd[i : i + 1] + even[i + 1 : i + 2]
    return merged


def sort_wires(wires, out):
    if len(wires) <= 2:
        return wires
    half = (len(wires) + 2) // 4 * 2
    return merge_wires(sort_wires(wires[:half], out), sort_wires(wires[half:], out), out)


def pruned(pairs, keep):
    needed = set(keep)
    kept = []
    for i, j in reversed(pairs):
        if i in needed or j in needed:
            kept.append((i, j, i in needed, j in needed))
            needed |= {i, j}
    return kept[::-1]


BLOCKS = (1, 3, 0, 2)
LEVELS = 2
PLANE = offsets(MEMBER)
NEAR = [o for o in PLANE if o["member_0"] == 0 or o["member_1"] == 0]
SIDE = [o for o in NEAR if o["member_1"] == 0 and o["member_2"] == 0]
FAR = [o for o in PLANE if o not in NEAR]
XY2 = [o for o in NEAR if chip_hops(o) == 2]
C1 = [o for o in NEAR if chip_hops(o) == 0]
D11 = [o for o in FAR if chip_hops(o) == 2]
D3 = [o for o in FAR if chip_hops(o) == 3]
D22 = [o for o in FAR if chip_hops(o) == 4]
N1 = [o for o in NEAR if chip_hops(o) == 1]
ROUNDS = (N1, C1 + D3 + D22, D11 + XY2)
SLOTS = N1 + C1 + D3 + D11 + D22 + XY2
GROUPS = (18, 8, 6)
RELAY = FAR[:2]
SECOND = 1
LINE = offsets(("lat",))
EVERYONE = offsets(AXES)


def sort_into(vals, pairs):
    for i, j, want_low, want_high in pairs:
        a, b = vals[i], vals[j]
        vals[i] = jnp.minimum(a, b) if want_low else None
        vals[j] = jnp.maximum(a, b) if want_high else None


def kernel(
    ens, obs, mask, band, crps_out, score_out,
    xv, ov, sbuf, rbuf, obuf, cbuf, asend, abuf, mask_s,
    load_sem, obs_sem, flag_sem, send_sem, recv_sem, relay_sem, asend_sem, arecv_sem, ready_sem, line_sem, hop_sem,
):
    here = {a: lax.axis_index(a) for a in AXES}
    me = member_of(here)

    mask_load = pltpu.make_async_copy(mask, mask_s, flag_sem)
    mask_load.start()
    for k, dx in enumerate(BLOCKS):
        first = pl.multiple_of(lax.rem(here["member_0"] + dx, 4) * 8, 8)
        load = pltpu.make_async_copy(ens.at[:, :, 0, pl.ds(first, 8)], xv.at[k], load_sem)
        load.start()

    barrier = pltpu.get_barrier_semaphore()
    for off in NEAR:
        pl.semaphore_signal(barrier, inc=1, device_id=peer(off), device_id_type=MESH_ID)
    last = here["lat"] // (SIZES["lat"] - 1)
    late = here["lat"] // 2
    mirror = SIZES["lat"] - 1 - here["lat"]

    @pl.when(last == 0)
    def _():
        up = dict(here, lat=SIZES["lat"] - 1)
        pl.semaphore_signal(barrier, inc=1, device_id=up, device_id_type=MESH_ID)

    @pl.when(here["lat"] == 1)
    def _():
        up = dict(here, lat=2)
        pl.semaphore_signal(barrier, inc=1, device_id=up, device_id_type=MESH_ID)

    tile_row = pl.multiple_of((me // 8) * 8, 8)
    obs_load = pltpu.make_async_copy(obs.at[:, 0, pl.ds(tile_row, 8)], ov, obs_sem)
    obs_load.start()

    pl.semaphore_wait(barrier, len(NEAR) + len(LINE) * last + (late - last))

    def pass_on(level):
        for off in SIDE:
            pl.semaphore_signal(
                hop_sem.at[level], inc=1, device_id=peer(off), device_id_type=MESH_ID
            )

    pass_on(0)

    @pl.when(last == 1)
    def _():
        for off in LINE:
            pl.semaphore_signal(line_sem, inc=1, device_id=peer(off), device_id_type=MESH_ID)
    mask_load.wait()
    pltpu.make_async_copy(xv, xv, load_sem).wait()
    flags = [mask_s[m].astype(jnp.float32) for m in range(2)]
    fills = [(1.0 - f) * BIG for f in flags]
    lane = lax.broadcasted_iota(jnp.int32, (8, LANES), 1)
    for k, dx in enumerate(BLOCKS):
        base = lax.rem(here["member_0"] + dx, 4) * (8 * S_STRIDE)

        def put(row, low, high):
            start = base + 2 * row
            sbuf[pl.ds(start, 8, stride=S_STRIDE), :] = low
            sbuf[pl.ds(start + 1, 8, stride=S_STRIDE), :] = high

        tails = []
        for v in range(VARS):
            for c in range(FULL + 1):
                width = LANES if c < FULL else TAIL
                pair = [
                    xv[k, m, v, :, pl.ds(c * LANES, width)] * flags[m] + fills[m] for m in range(2)
                ]
                low, high = jnp.minimum(*pair), jnp.maximum(*pair)
                if c < FULL:
                    put(v * FULL + c, low, high)
                else:
                    tails.append((low, high))
        rest = jnp.zeros((8, LANES - VARS * TAIL), jnp.float32)
        put(
            VARS * FULL,
            jnp.concatenate([p[0] for p in tails] + [rest], axis=1),
            jnp.concatenate([p[1] for p in tails] + [rest], axis=1),
        )

    own = pl.multiple_of(me * S_STRIDE, 8)
    rbuf[pl.ds(0, S_STRIDE), :] = sbuf[pl.ds(own, S_STRIDE), :]
    slots = {}

    def block(place):
        return pl.ds(pl.multiple_of(place * R_STRIDE, 8), SENT)

    def await_slots(flag, count):
        rows = rbuf.at[pl.ds(0, count * SENT)]
        pltpu.make_async_copy(rows, rows, recv_sem.at[flag]).wait()

    def send(group):
        for off in group:
            target = peer(off)
            start = pl.multiple_of(member_of(target) * S_STRIDE, 8)
            slot = slots[str(off)]
            place, flag = slot + 1, group_of(slot + 1)
            if off in RELAY:
                via = RELAY.index(off)
                moved = late if via < SECOND else last
                stop = dict(here, lat=mirror)
                target = {a: target[a] * (1 - moved) + stop[a] * moved for a in AXES}
                place = place * (1 - moved) + (32 + via) * moved
                flag = flag * (1 - moved) + (len(GROUPS) + via) * moved
            pltpu.make_async_remote_copy(
                src_ref=sbuf.at[pl.ds(start, SENT)],
                dst_ref=rbuf.at[block(place)],
                send_sem=send_sem,
                recv_sem=recv_sem.at[flag],
                device_id=target,
                device_id_type=MESH_ID,
            ).start()

    for level, group in enumerate(ROUNDS):
        if level == 1:
            pl.semaphore_wait(hop_sem.at[level - 1], len(SIDE))
            if level < LEVELS - 1:
                pass_on(level)
        for off in group:
            slots[str(off)] = SLOTS.index(off)
        if level < 2:
            send(group)

    early = 1 - late if SECOND else 1 - (here["lat"] + SIZES["lat"] - 1) // SIZES["lat"]

    @pl.when(early == 0)
    def _():
        send(ROUNDS[2])

    def forward(via):
        await_slots(len(GROUPS) + via, 1)
        slot = slots[str(RELAY[via])]
        pltpu.make_async_remote_copy(
            src_ref=rbuf.at[block(32 + via)],
            dst_ref=rbuf.at[block(slot + 1)],
            send_sem=relay_sem.at[via],
            recv_sem=recv_sem.at[group_of(slot + 1)],
            device_id=dict(peer(RELAY[via]), lat=mirror),
            device_id_type=MESH_ID,
        ).start()

    @pl.when(early == 1)
    def _():
        for via in range(SECOND):
            forward(via)

        @pl.when(here["lat"] == 0)
        def _():
            for via in range(SECOND, len(RELAY)):
                forward(via)

        send(ROUNDS[2])

    @pl.when(last == 0)
    def _():
        pl.semaphore_wait(line_sem, 1)

    for off in LINE:
        pl.semaphore_signal(ready_sem, inc=1, device_id=peer(off), device_id_type=MESH_ID)

    obs_load.wait()
    sub = lax.broadcasted_iota(jnp.int32, (8, LANES), 0)
    chosen = sub == lax.rem(me, 8)
    obs_tails = []
    for v in range(VARS):
        for c in range(FULL):
            part = jnp.where(chosen, ov[v, :, pl.ds(c * LANES, LANES)], 0.0)
            obuf[pl.ds(v * FULL + c, 1), :] = jnp.sum(part, axis=0, keepdims=True)
        part = jnp.where(chosen[:, :TAIL], ov[v, :, pl.ds(FULL * LANES, TAIL)], 0.0)
        obs_tails.append(jnp.sum(part, axis=0, keepdims=True))
    rest = jnp.zeros((1, LANES - VARS * TAIL), jnp.float32)
    obuf[pl.ds(VARS * FULL, 1), :] = jnp.concatenate(obs_tails + [rest], axis=1)
    global_row = (band[0] + me).astype(jnp.float32)
    angle = (90.0 - jnp.full((1, LANES), global_row) * 180.0 / (GRID_LAT - 1)) * math.pi / 180.0
    weight = jnp.cos(angle)

    def rows_of(q, k):
        return pl.ds((k // 2) * R_STRIDE + 16 * q + k % 2, 8, stride=2)

    order, done = [], 0
    for flag, count in enumerate(GROUPS):
        await_slots(flag, count if done else count - 1)
        stage = []
        fresh = list(range(2 * done, 2 * (done + count)))
        order = merge_wires(order, sort_wires(fresh, stage), stage)
        done += count
        if done == 32:
            break
        stage = pruned(stage, order)

        def presort(q, carry, stage=stage, wires=range(2 * done)):
            vals = [rbuf[rows_of(q, k), :] for k in wires]
            sort_into(vals, stage)
            for k in wires:
                rbuf[rows_of(q, k), :] = vals[k]
            return carry

        lax.fori_loop(0, COLS, presort, 0)

    order = order[:VALID]
    stage = pruned(stage, order)

    def column(q, sums):
        vals = [rbuf[rows_of(q, k), :] for k in range(64)]
        sort_into(vals, stage)
        truth = obuf[pl.ds(pl.multiple_of(8 * q, 8), 8), :]
        skill = [jnp.zeros((8, LANES), jnp.float32) for _ in range(2)]
        spread = [jnp.zeros((8, LANES), jnp.float32) for _ in range(2)]
        for k in range(VALID // 2):
            low, high = vals[order[k]], vals[order[VALID - 1 - k]]
            skill[0] = skill[0] + jnp.abs(low - truth)
            skill[1] = skill[1] + jnp.abs(high - truth)
            spread[k % 2] = spread[k % 2] + (high - low) * float(VALID - 1 - 2 * k)
        crps = (skill[0] + skill[1]) * (1.0 / VALID) - (spread[0] + spread[1]) * (
            1.0 / (VALID * (VALID - 1.0))
        )
        cbuf[pl.ds(pl.multiple_of(8 * q, 8), 8), :] = crps
        row = sub + 8 * q
        result = []
        for v in range(VARS):
            inside = (row >= v * FULL) & (row < (v + 1) * FULL)
            in_tail = (row == VARS * FULL) & (lane >= v * TAIL) & (lane < (v + 1) * TAIL)
            result.append(sums[v] + jnp.where(inside | in_tail, crps, 0.0))
        return tuple(result)

    sums = lax.fori_loop(
        0, COLS, column, tuple(jnp.zeros((8, LANES), jnp.float32) for _ in range(VARS)), unroll=True
    )
    totals = [jnp.sum(s, axis=(0, 1), keepdims=True) for s in sums]
    one_lane = lax.broadcasted_iota(jnp.int32, (1, LANES), 1)
    message = jnp.zeros((1, LANES), jnp.float32)
    for v in range(VARS):
        message = jnp.where(one_lane == v, totals[v] * weight, message)
    my_id = here["lat"] * 32 + me
    asend[0] = message
    abuf[my_id] = message

    pl.semaphore_wait(ready_sem, len(LINE))
    targets = [dict(peer(off), lat=z) for z in range(SIZES["lat"]) for off in PLANE]
    for target in targets + [peer(off) for off in LINE]:
        pltpu.make_async_remote_copy(
            src_ref=asend.at[0],
            dst_ref=abuf.at[my_id],
            send_sem=asend_sem,
            recv_sem=arecv_sem,
            device_id=target,
            device_id_type=MESH_ID,
        ).start()

    for v in range(VARS):
        for c in range(FULL):
            crps_out[v, 0, :, pl.ds(c * LANES, LANES)] = cbuf[pl.ds(v * FULL + c, 1), :]
        last = cbuf[pl.ds(VARS * FULL, 1), :]
        crps_out[v, 0, :, pl.ds(FULL * LANES, TAIL)] = last[:, v * TAIL : (v + 1) * TAIL]

    sent = sbuf.at[pl.ds(0, len(PLANE) * SENT)]
    pltpu.make_async_copy(sent, sent, send_sem).wait()
    relayed = rbuf.at[pl.ds(0, SENT)]
    for via in range(len(RELAY)):

        @pl.when(here["lat"] <= (1 if via < SECOND else 0))
        def _():
            pltpu.make_async_copy(relayed, relayed, relay_sem.at[via]).wait()

    arrived = abuf.at[pl.ds(0, len(EVERYONE))]
    pltpu.make_async_copy(arrived, arrived, arecv_sem).wait()
    total = jnp.sum(abuf[:, 0, :], axis=0, keepdims=True) * (1.0 / (4 * 32 * GRID_LON))
    score_out[...] = total
    pltpu.make_async_copy(arrived, arrived, asend_sem).wait()


def write_kernel(crps, score, crps_out, score_out):
    crps_out[...] = crps[...]
    score_out[...] = score[:, :VARS]


def on_device(ensemble, observation, valid_mask, band_start):
    vmem = pl.BlockSpec(memory_space=pltpu.VMEM)
    hbm = pl.BlockSpec(memory_space=pltpu.HBM)
    smem = pl.BlockSpec(memory_space=pltpu.SMEM)
    in_hbm = [
        pltpu.with_memory_space_constraint(a, pltpu.HBM)
        for a in (ensemble, observation, valid_mask)
    ]
    field = jax.ShapeDtypeStruct((VARS, 1, 1, GRID_LON), jnp.float32)
    crps_field, score = pl.pallas_call(
        kernel,
        out_shape=(field, jax.ShapeDtypeStruct((1, LANES), jnp.float32)),
        in_specs=[hbm, hbm, hbm, smem],
        out_specs=(vmem, vmem),
        scratch_shapes=[
            pltpu.VMEM((4, 2, VARS, 8, GRID_LON), jnp.float32),
            pltpu.VMEM((VARS, 8, GRID_LON), jnp.float32),
            pltpu.VMEM((32 * S_STRIDE, LANES), jnp.float32),
            pltpu.VMEM(((32 + len(RELAY)) * R_STRIDE, LANES), jnp.float32),
            pltpu.VMEM((8 * COLS, LANES), jnp.float32),
            pltpu.VMEM((8 * COLS, LANES), jnp.float32),
            pltpu.VMEM((1, 1, LANES), jnp.float32),
            pltpu.VMEM((128, 1, LANES), jnp.float32),
            pltpu.SMEM((2,), jnp.int32),
            pltpu.SemaphoreType.DMA,
            pltpu.SemaphoreType.DMA,
            pltpu.SemaphoreType.DMA,
            pltpu.SemaphoreType.DMA,
            pltpu.SemaphoreType.DMA((len(GROUPS) + len(RELAY),)),
            pltpu.SemaphoreType.DMA((len(RELAY),)),
            pltpu.SemaphoreType.DMA,
            pltpu.SemaphoreType.DMA,
            pltpu.SemaphoreType.REGULAR,
            pltpu.SemaphoreType.REGULAR,
            pltpu.SemaphoreType.REGULAR((LEVELS - 1,)),
        ],
        compiler_params=pltpu.CompilerParams(
            collective_id=0, has_side_effects=True, vmem_limit_bytes=8 * 1024 * 1024
        ),
        name="crps",
    )(*in_hbm, band_start)
    crps_field, score = pl.pallas_call(
        write_kernel,
        out_shape=(field, jax.ShapeDtypeStruct((1, VARS), jnp.float32)),
        in_specs=[vmem, vmem],
        out_specs=(vmem, vmem),
        compiler_params=pltpu.CompilerParams(vmem_limit_bytes=1024 * 1024),
        name="write",
    )(crps_field, score)
    return crps_field, score.reshape(VARS, 1)


def solution(mesh):
    torus = Mesh(
        mesh.devices.reshape(4, 4, 2, mesh.shape["lat"]),
        ("member_0", "member_1", "member_2", "lat"),
    )
    in_specs = (P(MEMBER, None, None, "lat", None), P(None, None, "lat", None), P(MEMBER), P("lat"))
    out_specs = (P(None, None, LAT_MEMBER, None), P())
    return jax.shard_map(
        on_device, mesh=torus, in_specs=in_specs, out_specs=out_specs, check_vma=False
    )
```

```python
import functools
import math

import jax
import jax.numpy as jnp
from jax import lax
from jax.experimental import pallas as pl
from jax.experimental.pallas import tpu as pltpu
from jax.sharding import Mesh
from jax.sharding import PartitionSpec as P

GRID_LAT = 721
GRID_LON = 1440
VALID = 50
BIG = 1.0e30
MEMBER = ("member_0", "member_1", "member_2")
LAT_MEMBER = ("lat", "member_0", "member_1", "member_2")
AXES = ("member_0", "member_1", "member_2", "lat")
SIZES = {"member_0": 4, "member_1": 4, "member_2": 2, "lat": 4}
MESH_ID = pl.DeviceIdType.MESH

LANES = 128
VARS = 3
FULL = GRID_LON // LANES
TAIL = GRID_LON - FULL * LANES
ROWS = VARS * FULL + 1
SENT = 2 * ROWS
S_STRIDE = 72
R_STRIDE = 80
COLS = 5


def offsets(axes):
    found = [{}]
    for axis in axes:
        found = [dict(o, **{axis: k}) for o in found for k in range(SIZES[axis])]
    found = [o for o in found if any(o.values())]

    def hops(o):
        return sum(min(k, SIZES[a] - k) if a != "member_2" else 0.3 * k for a, k in o.items())

    return sorted(found, key=lambda o: -hops(o))


def chip_hops(o):
    return sum(min(o[a], SIZES[a] - o[a]) for a in ("member_0", "member_1"))


def group_of(place):
    return 0 if place < GROUPS[0] else 1 if place < GROUPS[0] + GROUPS[1] else 2


def peer(offset):
    return {a: lax.rem(lax.axis_index(a) + offset.get(a, 0), SIZES[a]) for a in AXES}


def member_of(coords):
    return (coords["member_0"] * 4 + coords["member_1"]) * 2 + coords["member_2"]


def merge_wires(a, b, out):
    if not a or not b:
        return a + b
    if len(a) == 1 and len(b) == 1:
        out.append((a[0], b[0]))
        return [a[0], b[0]]
    even = merge_wires(a[0::2], b[0::2], out)
    odd = merge_wires(a[1::2], b[1::2], out)
    merged = even[:1]
    for i in range(max(len(odd), len(even) - 1)):
        if i < len(odd) and i + 1 < len(even):
            out.append((odd[i], even[i + 1]))
        merged += odd[i : i + 1] + even[i + 1 : i + 2]
    return merged


def sort_wires(wires, out):
    if len(wires) <= 2:
        return wires
    half = (len(wires) + 2) // 4 * 2
    return merge_wires(sort_wires(wires[:half], out), sort_wires(wires[half:], out), out)


def pruned(pairs, keep):
    needed = set(keep)
    kept = []
    for i, j in reversed(pairs):
        if i in needed or j in needed:
            kept.append((i, j, i in needed, j in needed))
            needed |= {i, j}
    return kept[::-1]


BLOCKS = (1, 3, 0, 2)
LEVELS = 2
PLANE = offsets(MEMBER)
NEAR = [o for o in PLANE if o["member_0"] == 0 or o["member_1"] == 0]
SIDE = [o for o in NEAR if o["member_1"] == 0 and o["member_2"] == 0]
FAR = [o for o in PLANE if o not in NEAR]
XY2 = [o for o in NEAR if chip_hops(o) == 2]
C1 = [o for o in NEAR if chip_hops(o) == 0]
D11 = [o for o in FAR if chip_hops(o) == 2]
D3 = [o for o in FAR if chip_hops(o) == 3]
D22 = [o for o in FAR if chip_hops(o) == 4]
N1 = [o for o in NEAR if chip_hops(o) == 1]
ROUNDS = (N1, C1 + D3 + D22, D11 + XY2)
SLOTS = N1 + C1 + D3 + D11 + D22 + XY2
GROUPS = (16, 10, 6)
RELAY = FAR[:2]
SECOND = 1
LINE = offsets(("lat",))
EVERYONE = offsets(AXES)


def sort_into(vals, pairs):
    for i, j, want_low, want_high in pairs:
        a, b = vals[i], vals[j]
        vals[i] = jnp.minimum(a, b) if want_low else None
        vals[j] = jnp.maximum(a, b) if want_high else None


def kernel(
    ens, obs, mask, band, crps_out, score_out,
    xv, ov, sbuf, rbuf, obuf, cbuf, asend, abuf, mask_s,
    load_sem, obs_sem, flag_sem, send_sem, recv_sem, relay_sem, asend_sem, arecv_sem, ready_sem, line_sem, hop_sem,
):
    here = {a: lax.axis_index(a) for a in AXES}
    me = member_of(here)

    mask_load = pltpu.make_async_copy(mask, mask_s, flag_sem)
    mask_load.start()
    for k, dx in enumerate(BLOCKS):
        first = pl.multiple_of(lax.rem(here["member_0"] + dx, 4) * 8, 8)
        load = pltpu.make_async_copy(ens.at[:, :, 0, pl.ds(first, 8)], xv.at[k], load_sem)
        load.start()

    barrier = pltpu.get_barrier_semaphore()
    for off in NEAR:
        pl.semaphore_signal(barrier, inc=1, device_id=peer(off), device_id_type=MESH_ID)
    last = here["lat"] // (SIZES["lat"] - 1)
    late = here["lat"] // 2
    mirror = SIZES["lat"] - 1 - here["lat"]

    @pl.when(last == 0)
    def _():
        up = dict(here, lat=SIZES["lat"] - 1)
        pl.semaphore_signal(barrier, inc=1, device_id=up, device_id_type=MESH_ID)

    @pl.when(here["lat"] == 1)
    def _():
        up = dict(here, lat=2)
        pl.semaphore_signal(barrier, inc=1, device_id=up, device_id_type=MESH_ID)

    tile_row = pl.multiple_of((me // 8) * 8, 8)
    obs_load = pltpu.make_async_copy(obs.at[:, 0, pl.ds(tile_row, 8)], ov, obs_sem)
    obs_load.start()

    pl.semaphore_wait(barrier, len(NEAR) + len(LINE) * last + (late - last))

    def pass_on(level):
        for off in SIDE:
            pl.semaphore_signal(
                hop_sem.at[level], inc=1, device_id=peer(off), device_id_type=MESH_ID
            )

    pass_on(0)

    @pl.when(last == 1)
    def _():
        for off in LINE:
            pl.semaphore_signal(line_sem, inc=1, device_id=peer(off), device_id_type=MESH_ID)
    mask_load.wait()
    pltpu.make_async_copy(xv, xv, load_sem).wait()
    flags = [mask_s[m].astype(jnp.float32) for m in range(2)]
    fills = [(1.0 - f) * BIG for f in flags]
    lane = lax.broadcasted_iota(jnp.int32, (8, LANES), 1)
    for k, dx in enumerate(BLOCKS):
        base = lax.rem(here["member_0"] + dx, 4) * (8 * S_STRIDE)

        def put(row, low, high):
            start = base + 2 * row
            sbuf[pl.ds(start, 8, stride=S_STRIDE), :] = low
            sbuf[pl.ds(start + 1, 8, stride=S_STRIDE), :] = high

        tails = []
        for v in range(VARS):
            for c in range(FULL + 1):
                width = LANES if c < FULL else TAIL
                pair = [
                    xv[k, m, v, :, pl.ds(c * LANES, width)] * flags[m] + fills[m] for m in range(2)
                ]
                low, high = jnp.minimum(*pair), jnp.maximum(*pair)
                if c < FULL:
                    put(v * FULL + c, low, high)
                else:
                    tails.append((low, high))
        rest = jnp.zeros((8, LANES - VARS * TAIL), jnp.float32)
        put(
            VARS * FULL,
            jnp.concatenate([p[0] for p in tails] + [rest], axis=1),
            jnp.concatenate([p[1] for p in tails] + [rest], axis=1),
        )

    own = pl.multiple_of(me * S_STRIDE, 8)
    rbuf[pl.ds(0, S_STRIDE), :] = sbuf[pl.ds(own, S_STRIDE), :]
    slots = {}

    def block(place):
        return pl.ds(pl.multiple_of(place * R_STRIDE, 8), SENT)

    def await_slots(flag, count):
        rows = rbuf.at[pl.ds(0, count * SENT)]
        pltpu.make_async_copy(rows, rows, recv_sem.at[flag]).wait()

    def send(group):
        for off in group:
            target = peer(off)
            start = pl.multiple_of(member_of(target) * S_STRIDE, 8)
            slot = slots[str(off)]
            place, flag = slot + 1, group_of(slot + 1)
            if off in RELAY:
                via = RELAY.index(off)
                moved = late if via < SECOND else last
                stop = dict(here, lat=mirror)
                target = {a: target[a] * (1 - moved) + stop[a] * moved for a in AXES}
                place = place * (1 - moved) + (32 + via) * moved
                flag = flag * (1 - moved) + (len(GROUPS) + via) * moved
            pltpu.make_async_remote_copy(
                src_ref=sbuf.at[pl.ds(start, SENT)],
                dst_ref=rbuf.at[block(place)],
                send_sem=send_sem,
                recv_sem=recv_sem.at[flag],
                device_id=target,
                device_id_type=MESH_ID,
            ).start()

    for level, group in enumerate(ROUNDS):
        if level == 1:
            pl.semaphore_wait(hop_sem.at[level - 1], len(SIDE))
            if level < LEVELS - 1:
                pass_on(level)
        for off in group:
            slots[str(off)] = SLOTS.index(off)
        if level < 2:
            send(group)

    early = 1 - late if SECOND else 1 - (here["lat"] + SIZES["lat"] - 1) // SIZES["lat"]

    @pl.when(early == 0)
    def _():
        send(ROUNDS[2])

    def forward(via):
        await_slots(len(GROUPS) + via, 1)
        slot = slots[str(RELAY[via])]
        pltpu.make_async_remote_copy(
            src_ref=rbuf.at[block(32 + via)],
            dst_ref=rbuf.at[block(slot + 1)],
            send_sem=relay_sem.at[via],
            recv_sem=recv_sem.at[group_of(slot + 1)],
            device_id=dict(peer(RELAY[via]), lat=mirror),
            device_id_type=MESH_ID,
        ).start()

    @pl.when(early == 1)
    def _():
        for via in range(SECOND):
            forward(via)

        @pl.when(here["lat"] == 0)
        def _():
            for via in range(SECOND, len(RELAY)):
                forward(via)

        send(ROUNDS[2])

    @pl.when(last == 0)
    def _():
        pl.semaphore_wait(line_sem, 1)

    for off in LINE:
        pl.semaphore_signal(ready_sem, inc=1, device_id=peer(off), device_id_type=MESH_ID)

    obs_load.wait()
    sub = lax.broadcasted_iota(jnp.int32, (8, LANES), 0)
    chosen = sub == lax.rem(me, 8)
    obs_tails = []
    for v in range(VARS):
        for c in range(FULL):
            part = jnp.where(chosen, ov[v, :, pl.ds(c * LANES, LANES)], 0.0)
            obuf[pl.ds(v * FULL + c, 1), :] = jnp.sum(part, axis=0, keepdims=True)
        part = jnp.where(chosen[:, :TAIL], ov[v, :, pl.ds(FULL * LANES, TAIL)], 0.0)
        obs_tails.append(jnp.sum(part, axis=0, keepdims=True))
    rest = jnp.zeros((1, LANES - VARS * TAIL), jnp.float32)
    obuf[pl.ds(VARS * FULL, 1), :] = jnp.concatenate(obs_tails + [rest], axis=1)
    global_row = (band[0] + me).astype(jnp.float32)
    angle = (90.0 - jnp.full((1, LANES), global_row) * 180.0 / (GRID_LAT - 1)) * math.pi / 180.0
    weight = jnp.cos(angle)

    def rows_of(q, k):
        return pl.ds((k // 2) * R_STRIDE + 16 * q + k % 2, 8, stride=2)

    order, done = [], 0
    for flag, count in enumerate(GROUPS):
        await_slots(flag, count if done else count - 1)
        stage = []
        fresh = list(range(2 * done, 2 * (done + count)))
        order = merge_wires(order, sort_wires(fresh, stage), stage)
        done += count
        if done == 32:
            break
        stage = pruned(stage, order)

        def presort(q, carry, stage=stage, wires=range(2 * done)):
            vals = [rbuf[rows_of(q, k), :] for k in wires]
            sort_into(vals, stage)
            for k in wires:
                rbuf[rows_of(q, k), :] = vals[k]
            return carry

        lax.fori_loop(0, COLS, presort, 0)

    order = order[:VALID]
    stage = pruned(stage, order)

    def column(q, sums):
        vals = [rbuf[rows_of(q, k), :] for k in range(64)]
        sort_into(vals, stage)
        truth = obuf[pl.ds(pl.multiple_of(8 * q, 8), 8), :]
        skill = [jnp.zeros((8, LANES), jnp.float32) for _ in range(2)]
        spread = [jnp.zeros((8, LANES), jnp.float32) for _ in range(2)]
        for k in range(VALID // 2):
            low, high = vals[order[k]], vals[order[VALID - 1 - k]]
            skill[0] = skill[0] + jnp.abs(low - truth)
            skill[1] = skill[1] + jnp.abs(high - truth)
            spread[k % 2] = spread[k % 2] + (high - low) * float(VALID - 1 - 2 * k)
        crps = (skill[0] + skill[1]) * (1.0 / VALID) - (spread[0] + spread[1]) * (
            1.0 / (VALID * (VALID - 1.0))
        )
        cbuf[pl.ds(pl.multiple_of(8 * q, 8), 8), :] = crps
        row = sub + 8 * q
        result = []
        for v in range(VARS):
            inside = (row >= v * FULL) & (row < (v + 1) * FULL)
            in_tail = (row == VARS * FULL) & (lane >= v * TAIL) & (lane < (v + 1) * TAIL)
            result.append(sums[v] + jnp.where(inside | in_tail, crps, 0.0))
        return tuple(result)

    sums = lax.fori_loop(
        0, COLS, column, tuple(jnp.zeros((8, LANES), jnp.float32) for _ in range(VARS))
    )
    totals = [jnp.sum(s, axis=(0, 1), keepdims=True) for s in sums]
    one_lane = lax.broadcasted_iota(jnp.int32, (1, LANES), 1)
    message = jnp.zeros((1, LANES), jnp.float32)
    for v in range(VARS):
        message = jnp.where(one_lane == v, totals[v] * weight, message)
    my_id = here["lat"] * 32 + me
    asend[0] = message
    abuf[my_id] = message

    pl.semaphore_wait(ready_sem, len(LINE))
    targets = [dict(peer(off), lat=z) for z in range(SIZES["lat"]) for off in PLANE]
    for target in targets + [peer(off) for off in LINE]:
        pltpu.make_async_remote_copy(
            src_ref=asend.at[0],
            dst_ref=abuf.at[my_id],
            send_sem=asend_sem,
            recv_sem=arecv_sem,
            device_id=target,
            device_id_type=MESH_ID,
        ).start()

    for v in range(VARS):
        for c in range(FULL):
            crps_out[v, 0, :, pl.ds(c * LANES, LANES)] = cbuf[pl.ds(v * FULL + c, 1), :]
        last = cbuf[pl.ds(VARS * FULL, 1), :]
        crps_out[v, 0, :, pl.ds(FULL * LANES, TAIL)] = last[:, v * TAIL : (v + 1) * TAIL]

    sent = sbuf.at[pl.ds(0, len(PLANE) * SENT)]
    pltpu.make_async_copy(sent, sent, send_sem).wait()
    relayed = rbuf.at[pl.ds(0, SENT)]
    for via in range(len(RELAY)):

        @pl.when(here["lat"] <= (1 if via < SECOND else 0))
        def _():
            pltpu.make_async_copy(relayed, relayed, relay_sem.at[via]).wait()

    arrived = abuf.at[pl.ds(0, len(EVERYONE))]
    pltpu.make_async_copy(arrived, arrived, arecv_sem).wait()
    total = jnp.sum(abuf[:, 0, :], axis=0, keepdims=True) * (1.0 / (4 * 32 * GRID_LON))
    score_out[...] = total
    pltpu.make_async_copy(arrived, arrived, asend_sem).wait()


def write_kernel(crps, score, crps_out, score_out):
    crps_out[...] = crps[...]
    score_out[...] = score[:, :VARS]


def on_device(ensemble, observation, valid_mask, band_start):
    vmem = pl.BlockSpec(memory_space=pltpu.VMEM)
    hbm = pl.BlockSpec(memory_space=pltpu.HBM)
    smem = pl.BlockSpec(memory_space=pltpu.SMEM)
    in_hbm = [
        pltpu.with_memory_space_constraint(a, pltpu.HBM)
        for a in (ensemble, observation, valid_mask)
    ]
    field = jax.ShapeDtypeStruct((VARS, 1, 1, GRID_LON), jnp.float32)
    crps_field, score = pl.pallas_call(
        kernel,
        out_shape=(field, jax.ShapeDtypeStruct((1, LANES), jnp.float32)),
        in_specs=[hbm, hbm, hbm, smem],
        out_specs=(vmem, vmem),
        scratch_shapes=[
            pltpu.VMEM((4, 2, VARS, 8, GRID_LON), jnp.float32),
            pltpu.VMEM((VARS, 8, GRID_LON), jnp.float32),
            pltpu.VMEM((32 * S_STRIDE, LANES), jnp.float32),
            pltpu.VMEM(((32 + len(RELAY)) * R_STRIDE, LANES), jnp.float32),
            pltpu.VMEM((8 * COLS, LANES), jnp.float32),
            pltpu.VMEM((8 * COLS, LANES), jnp.float32),
            pltpu.VMEM((1, 1, LANES), jnp.float32),
            pltpu.VMEM((128, 1, LANES), jnp.float32),
            pltpu.SMEM((2,), jnp.int32),
            pltpu.SemaphoreType.DMA,
            pltpu.SemaphoreType.DMA,
            pltpu.SemaphoreType.DMA,
            pltpu.SemaphoreType.DMA,
            pltpu.SemaphoreType.DMA((len(GROUPS) + len(RELAY),)),
            pltpu.SemaphoreType.DMA((len(RELAY),)),
            pltpu.SemaphoreType.DMA,
            pltpu.SemaphoreType.DMA,
            pltpu.SemaphoreType.REGULAR,
            pltpu.SemaphoreType.REGULAR,
            pltpu.SemaphoreType.REGULAR((LEVELS - 1,)),
        ],
        compiler_params=pltpu.CompilerParams(
            collective_id=0, has_side_effects=True, vmem_limit_bytes=8 * 1024 * 1024
        ),
        name="crps",
    )(*in_hbm, band_start)
    crps_field, score = pl.pallas_call(
        write_kernel,
        out_shape=(field, jax.ShapeDtypeStruct((1, VARS), jnp.float32)),
        in_specs=[vmem, vmem],
        out_specs=(vmem, vmem),
        compiler_params=pltpu.CompilerParams(vmem_limit_bytes=1024 * 1024),
        name="write",
    )(crps_field, score)
    return crps_field, score.reshape(VARS, 1)


def solution(mesh):
    torus = Mesh(
        mesh.devices.reshape(4, 4, 2, mesh.shape["lat"]),
        ("member_0", "member_1", "member_2", "lat"),
    )
    in_specs = (P(MEMBER, None, None, "lat", None), P(None, None, "lat", None), P(MEMBER), P("lat"))
    out_specs = (P(None, None, LAT_MEMBER, None), P())
    return jax.shard_map(
        on_device, mesh=torus, in_specs=in_specs, out_specs=out_specs, check_vma=False
    )
```
